32 devices in a mesh: dp: 8 (over z, y), tensor: 4 (over x, core).
Axes of the slice: x: 2, y: 2, z: 4, core: 2. Of those that a mesh axis runs over, the one named last changes fastest.
Arguments:
- block_input: bfloat16 [2, 1024, 8, 1024], P(None, 'tensor', 'dp'), may hold values from -6 to 6
- qkv_weight: bfloat16 [1024, 3, 1024], P('dp', None, 'tensor'), may hold values from -0.1875 to 0.1875
- qv_bias: float32 [2, 1024], P(None, 'tensor'), may hold values from -2 to 2
- out_weight: bfloat16 [1024, 1024], P('dp', 'tensor'), may hold values from -0.75 to 0.75
- out_bias: float32 [1024], replicated, may hold values from -2 to 2
- fc_weight: bfloat16 [1024, 4096], P('dp', 'tensor'), may hold values from -0.1875 to 0.1875
- fc_bias: float32 [4096], P('tensor'), may hold values from -2 to 2
- proj_weight: bfloat16 [1024, 4096], P('dp', 'tensor'), may hold values from -0.09375 to 0.09375
- proj_bias: float32 [1024], replicated, may hold values from -2 to 2
- norm1_gain: float32 [1024], replicated, may hold values from 0.1 to 1.9
- norm1_shift: float32 [1024], replicated, may hold values from -2 to 2
- norm2_gain: float32 [1024], replicated, may hold values from 0.1 to 1.9
- norm2_shift: float32 [1024], replicated, may hold values from -2 to 2
- out_grad: bfloat16 [2, 1024, 8, 1024], P(None, 'tensor', 'dp'), may hold values from -6 to 6
Outputs:
- block_output: bfloat16 [2, 1024, 8, 1024], P(None, 'tensor', 'dp')
- input_grad: bfloat16 [2, 1024, 8, 1024], P(None, 'tensor', 'dp')
- qkv_weight_grad: float32 [1024, 3, 1024], P('dp', None, 'tensor')
- qv_bias_grad: float32 [2, 1024], P(None, 'tensor')
- out_weight_grad: float32 [1024, 1024], P('dp', 'tensor')
- out_bias_grad: float32 [1024], replicated
- fc_weight_grad: float32 [1024, 4096], P('dp', 'tensor')
- fc_bias_grad: float32 [4096], P('tensor')
- proj_weight_grad: float32 [1024, 4096], P('dp', 'tensor')
- proj_bias_grad: float32 [1024], replicated
- norm1_gain_grad: float32 [1024], replicated
- norm1_shift_grad: float32 [1024], replicated
- norm2_gain_grad: float32 [1024], replicated
- norm2_shift_grad: float32 [1024], replicated
The draws below stay inside these ranges and needn't reach their ends.
All inputs are finite; a program needn't handle non-finite values.
Results may differ from the reference program's by a relative error of at most 0.012.
Values may be sent and summed in bfloat16 or wider, within the bound.
A program may use at most 128 MiB of HBM per device.

```python
import jax
import jax.numpy as jnp
from jax import lax

D = 1024
HEADS = 16
HEAD_DIM = 64
FF = 4096
SEQ_LEN = 1024
MICRO = 2
BATCH = 8


def level_of(rng, dims, split, low, top_value):
    factor_of, own = 1.0, jax.random.fold_in(rng, 6)
    for position, shards_of in split:
        heights = jnp.exp(jax.random.uniform(jax.random.fold_in(own, position), (shards_of,), jnp.float32, low / len(split), top_value / len(split)))
        factor_of = factor_of * jnp.repeat(heights, dims[position] // shards_of).reshape([-1 if axis == position else 1 for axis in range(len(dims))])
    return factor_of


def gaussian(own_key, dims, scale, limit, split=(), held_as=jnp.bfloat16):
    values = jax.random.normal(own_key, dims, jnp.float32) * scale
    if len(split) > 0:
        values = level_of(own_key, dims, split, -0.22, 0.18) * values
    return jnp.clip(values, min=-limit, max=limit).astype(held_as)


def setup_inputs(seed: int = 0) -> dict:
    splits = jax.random.split(jax.random.key(seed), 15)
    block_input = gaussian(splits[0], (MICRO, SEQ_LEN, BATCH, D), 1.0, 6.0, ((1, 4), (2, 8)))
    qkv_weight = gaussian(splits[1], (D, 3, D), D ** -0.5, 0.1875, ((0, 8), (2, 4)))
    qv_bias = gaussian(splits[2], (2, D), 0.3, 2.0, ((1, 4),), jnp.float32)
    out_weight = gaussian(splits[3], (D, D), (D // 16) ** -0.5, 0.75, ((0, 8), (1, 4)))
    out_bias = gaussian(splits[4], (D,), 0.3, 2.0, (), jnp.float32)
    fc_weight = gaussian(splits[5], (D, FF), D ** -0.5, 0.1875, ((0, 8), (1, 4)))
    fc_bias = gaussian(splits[6], (FF,), 0.3, 2.0, ((0, 4),), jnp.float32)
    proj_weight = gaussian(splits[7], (D, FF), FF ** -0.5, 0.09375, ((0, 8), (1, 4)))
    proj_bias = gaussian(splits[8], (D,), 0.3, 2.0, (), jnp.float32)
    norm1_gain = jnp.clip(1.0 + 0.18 * jax.random.normal(splits[9], (D,), jnp.float32), 0.1, 1.9)
    norm1_shift = gaussian(splits[10], (D,), 0.3, 2.0, (), jnp.float32)
    norm2_gain = jnp.clip(1.0 + 0.18 * jax.random.normal(splits[11], (D,), jnp.float32), 0.1, 1.9)
    norm2_shift = gaussian(splits[12], (D,), 0.3, 2.0, (), jnp.float32)
    out_grad = gaussian(splits[13], (MICRO, SEQ_LEN, BATCH, D), 1.0, 6.0, ((1, 4), (2, 8)))
    return dict(block_input=block_input, qkv_weight=qkv_weight, qv_bias=qv_bias, out_weight=out_weight, out_bias=out_bias, fc_weight=fc_weight, fc_bias=fc_bias, proj_weight=proj_weight, proj_bias=proj_bias, norm1_gain=norm1_gain, norm1_shift=norm1_shift, norm2_gain=norm2_gain, norm2_shift=norm2_shift, out_grad=out_grad)


@jax.custom_vjp
def low(v):
    return lax.optimization_barrier(v.astype(jnp.bfloat16)).astype(jnp.float32)

@jax.custom_vjp
def low_back(v):
    return v

def low_keep(v):
    return (low(v), None)

def low_pass(kept, grad):
    return (grad,)

def back_keep(v):
    return (v, None)

def back_low(kept, grad):
    return (low(grad),)
low.defvjp(low_keep, low_pass)
low_back.defvjp(back_keep, back_low)

def product(left, right, form):
    return jnp.einsum(form, left, right, precision=lax.Precision.HIGHEST)

def layer_norm(rows, gain, shift):
    center = rows - lax.optimization_barrier(jnp.mean(rows, axis=-1, keepdims=True))
    spread = lax.optimization_barrier(jnp.mean(center * center, axis=-1, keepdims=True))
    return center * lax.rsqrt(spread + 1e-05) * gain + shift

def gelu_tanh(values):
    return 0.5 * values * (1.0 + jnp.tanh(0.7978845608028654 * (values + 0.044715 * values * values * values)))

def block(params, rows):
    qkv_weight, qv_bias, out_weight, out_bias, fc_weight, fc_bias, proj_weight, proj_bias, norm1_gain, norm1_shift, norm2_gain, norm2_shift = params
    length = rows.shape[0]
    hidden1 = low(layer_norm(rows, norm1_gain, norm1_shift))
    queries = low(low_back(product(hidden1, qkv_weight[:, 0, :], 'ld,de->le') + qv_bias[0]))
    keys = low(low_back(product(hidden1, qkv_weight[:, 1, :], 'ld,de->le')))
    values = low(low_back(product(hidden1, qkv_weight[:, 2, :], 'ld,de->le') + qv_bias[1]))
    query_heads = queries.reshape(length, HEADS, HEAD_DIM)
    key_heads = keys.reshape(length, HEADS, HEAD_DIM)
    value_heads = values.reshape(length, HEADS, HEAD_DIM)
    scores = low_back(product(query_heads, key_heads, 'qhe,khe->hqk') * HEAD_DIM ** (-0.5))
    row_pos = lax.broadcasted_iota(jnp.int32, (length, length), 0)
    col_pos = lax.broadcasted_iota(jnp.int32, (length, length), 1)
    scores = jnp.where(col_pos <= row_pos, scores, -1e+30)
    peak = lax.optimization_barrier(jnp.max(scores, axis=-1, keepdims=True))
    raised = jnp.exp(scores - peak)
    probs = raised / lax.optimization_barrier(jnp.sum(raised, axis=-1, keepdims=True))
    attended = product(low(probs), value_heads, 'hqk,khe->qhe').reshape(length, HEADS * HEAD_DIM)
    mixed = low(low_back(attended))
    middle = rows + low_back(product(mixed, out_weight, 'li,oi->lo')) + out_bias
    hidden2 = low(layer_norm(middle, norm2_gain, norm2_shift))
    pre_act = low_back(product(hidden2, fc_weight, 'ld,df->lf') + fc_bias)
    activated = low(gelu_tanh(pre_act))
    return middle + low_back(product(activated, proj_weight, 'lf,of->lo')) + proj_bias

def reference(block_input, qkv_weight, qv_bias, out_weight, out_bias, fc_weight, fc_bias, proj_weight, proj_bias, norm1_gain, norm1_shift, norm2_gain, norm2_shift, out_grad):
    params = tuple((item.astype(jnp.float32) for item in (qkv_weight, qv_bias, out_weight, out_bias, fc_weight, fc_bias, proj_weight, proj_bias, norm1_gain, norm1_shift, norm2_gain, norm2_shift)))
    micro, length, batch, width = block_input.shape
    inputs_seq = jnp.transpose(block_input.astype(jnp.float32), (0, 2, 1, 3)).reshape(micro * batch, length, width)
    grads_seq = jnp.transpose(out_grad.astype(jnp.float32), (0, 2, 1, 3)).reshape(micro * batch, length, width)

    def one_sequence(totals, pair):
        rows, grad_rows = pair
        result, pull = jax.vjp(block, params, rows)
        grad_params, grad_in = pull(grad_rows)
        return (tuple((total + extra for total, extra in zip(totals, grad_params))), (result, grad_in))
    start = tuple((jnp.zeros_like(item) for item in params))
    totals, (results, grad_inputs) = lax.scan(one_sequence, start, (inputs_seq, grads_seq))
    outputs = jnp.transpose(results.reshape(micro, batch, length, width), (0, 2, 1, 3)).astype(jnp.bfloat16)
    in_grads = jnp.transpose(grad_inputs.reshape(micro, batch, length, width), (0, 2, 1, 3)).astype(jnp.bfloat16)
    return (outputs, in_grads, totals[0], totals[1], totals[2], totals[3], totals[4], totals[5], totals[6], totals[7], totals[8], totals[9], totals[10], totals[11])
```

```python
import jax
import jax.numpy as jnp
from jax import lax
from jax.sharding import PartitionSpec as P

HEAD_DIM = 64


norm_eps = 1e-05
tanh_coef = 0.7978845608028654
cube_coef = 0.044715
block_rows = 512


def gelu_tanh(values):
    return (
        0.5 * values * (1.0 + jnp.tanh(tanh_coef * (values + cube_coef * values * values * values)))
    )


def norm_parts(rows):
    center = rows - jnp.mean(rows, axis=-1, keepdims=True)
    spread = jnp.mean(center * center, axis=-1, keepdims=True)
    inverse = lax.rsqrt(spread + norm_eps)
    return (center * inverse, inverse)


def norm_back(grad_out, normed, inverse, gain):
    grad_normed = grad_out * gain
    first = jnp.mean(grad_normed, axis=-1, keepdims=True)
    second = jnp.mean(grad_normed * normed, axis=-1, keepdims=True)
    return inverse * (grad_normed - first - normed * second)


def causal_scores(query_block, keys, offset):
    scores = jnp.einsum(
        "qbhe,kbhe->bhqk", query_block, keys, preferred_element_type=jnp.float32
    ) * HEAD_DIM ** (-0.5)
    height = query_block.shape[0]
    length = keys.shape[0]
    row_pos = lax.broadcasted_iota(jnp.int32, (height, length), 0) + offset
    col_pos = lax.broadcasted_iota(jnp.int32, (height, length), 1)
    return jnp.where(col_pos <= row_pos, scores, -1e30)


def attend_forward(queries, keys, values):
    length = keys.shape[0]
    span = min(block_rows, length)
    outputs = []
    totals = []
    for offset in range(0, length, span):
        scores = causal_scores(queries[offset : offset + span], keys, offset)
        peak = jnp.max(scores, axis=-1, keepdims=True)
        raised = jnp.exp(scores - peak)
        total = jnp.sum(raised, axis=-1, keepdims=True)
        weights = (raised / total).astype(jnp.bfloat16)
        outputs.append(
            jnp.einsum("bhqk,kbhe->qbhe", weights, values, preferred_element_type=jnp.float32)
        )
        totals.append(peak + jnp.log(total))
    return (jnp.concatenate(outputs, 0), jnp.concatenate(totals, 2))


def attend_backward(queries, keys, values, log_totals, grad_out):
    length = keys.shape[0]
    span = min(block_rows, length)
    scale = HEAD_DIM ** (-0.5)
    grad_queries = []
    grad_keys = jnp.zeros(keys.shape, jnp.float32)
    grad_values = jnp.zeros(values.shape, jnp.float32)
    for offset in range(0, length, span):
        query_block = queries[offset : offset + span]
        grad_block = grad_out[offset : offset + span]
        scores = causal_scores(query_block, keys, offset)
        probs = jnp.exp(scores - log_totals[:, :, offset : offset + span])
        grad_probs = jnp.einsum(
            "qbhe,kbhe->bhqk", grad_block, values, preferred_element_type=jnp.float32
        )
        inner = jnp.sum(probs * grad_probs, axis=-1, keepdims=True)
        grad_scores = (probs * (grad_probs - inner)).astype(jnp.bfloat16)
        grad_queries.append(
            jnp.einsum("bhqk,kbhe->qbhe", grad_scores, keys, preferred_element_type=jnp.float32)
            * scale
        )
        grad_keys = (
            grad_keys
            + jnp.einsum(
                "bhqk,qbhe->kbhe", grad_scores, query_block, preferred_element_type=jnp.float32
            )
            * scale
        )
        grad_values = grad_values + jnp.einsum(
            "bhqk,qbhe->kbhe",
            probs.astype(jnp.bfloat16),
            grad_block,
            preferred_element_type=jnp.float32,
        )
    return (jnp.concatenate(grad_queries, 0), grad_keys, grad_values)


def per_device(
    block_input,
    qkv_weight,
    qv_bias,
    out_weight,
    out_bias,
    fc_weight,
    fc_bias,
    proj_weight,
    proj_bias,
    norm1_gain,
    norm1_shift,
    norm2_gain,
    norm2_shift,
    out_grad,
):
    micro = block_input.shape[0]
    heads_local = qkv_weight.shape[2] // HEAD_DIM
    rows = qkv_weight.shape[0]
    width_qkv = qkv_weight.shape[1] * qkv_weight.shape[2]
    width_out = out_weight.shape[1]
    width_fc = fc_weight.shape[1]
    cuts = (width_qkv, width_qkv + width_out, width_qkv + width_out + width_fc)
    packed = jnp.concatenate(
        [qkv_weight.reshape(rows, width_qkv), out_weight, fc_weight, proj_weight], axis=1
    )
    packed_full = lax.all_gather(packed, "dp", axis=0, tiled=True)
    depth = packed_full.shape[0]
    qkv_full = packed_full[:, : cuts[0]].reshape(depth, 3, qkv_weight.shape[2])
    out_full = packed_full[:, cuts[0] : cuts[1]]
    fc_full = packed_full[:, cuts[1] : cuts[2]]
    proj_full = packed_full[:, cuts[2] :]
    grad_top_all = lax.all_gather(out_grad, "tensor", axis=1, tiled=True)
    weight_init = jnp.zeros(packed_full.shape, jnp.float32)
    small_init = (
        jnp.zeros(qv_bias.shape, jnp.float32),
        jnp.zeros(fc_bias.shape, jnp.float32),
        jnp.zeros(out_bias.shape, jnp.float32),
        jnp.zeros(proj_bias.shape, jnp.float32),
        jnp.zeros(norm1_gain.shape, jnp.float32),
        jnp.zeros(norm1_shift.shape, jnp.float32),
        jnp.zeros(norm2_gain.shape, jnp.float32),
        jnp.zeros(norm2_shift.shape, jnp.float32),
    )
    outputs_init = jnp.zeros(block_input.shape, jnp.bfloat16)
    in_grads_init = jnp.zeros(block_input.shape, jnp.bfloat16)

    def one_micro(index, carry):
        outputs_all, in_grads_all, weight_acc, small_acc = carry
        resid_in = lax.dynamic_index_in_dim(block_input, index, 0, keepdims=False).astype(
            jnp.float32
        )
        grad_top = lax.dynamic_index_in_dim(out_grad, index, 0, keepdims=False)
        grad_top_full = lax.dynamic_index_in_dim(grad_top_all, index, 0, keepdims=False)
        normed1, inverse1 = norm_parts(resid_in)
        hidden1 = (normed1 * norm1_gain + norm1_shift).astype(jnp.bfloat16)
        hidden1_full = lax.all_gather(hidden1, "tensor", axis=0, tiled=True)
        length = hidden1_full.shape[0]
        batch = hidden1_full.shape[1]
        projected = jnp.einsum(
            "lbd,dce->lbce", hidden1_full, qkv_full, preferred_element_type=jnp.float32
        )
        qkv_bias = jnp.stack([qv_bias[0], jnp.zeros_like(qv_bias[0]), qv_bias[1]])
        qkv_values = (projected + qkv_bias).astype(jnp.bfloat16)
        split = qkv_values.reshape(length, batch, 3, heads_local, HEAD_DIM)
        queries = split[:, :, 0]
        keys = split[:, :, 1]
        values = split[:, :, 2]
        attended, log_totals = attend_forward(queries, keys, values)
        mixed = attended.astype(jnp.bfloat16).reshape(length, batch, heads_local * HEAD_DIM)
        attn_branch = lax.psum_scatter(
            jnp.einsum("lbi,oi->lbo", mixed, out_full, preferred_element_type=jnp.float32),
            "tensor",
            scatter_dimension=0,
            tiled=True,
        )
        middle = resid_in + attn_branch + out_bias
        normed2, inverse2 = norm_parts(middle)
        hidden2 = (normed2 * norm2_gain + norm2_shift).astype(jnp.bfloat16)
        hidden2_full = lax.all_gather(hidden2, "tensor", axis=0, tiled=True)
        pre_act = (
            jnp.einsum("lbd,df->lbf", hidden2_full, fc_full, preferred_element_type=jnp.float32)
            + fc_bias
        )
        activated = gelu_tanh(pre_act).astype(jnp.bfloat16)
        mlp_branch = lax.psum_scatter(
            jnp.einsum(
                "lbf,of->lbo", activated, proj_full, preferred_element_type=jnp.float32
            ).astype(jnp.bfloat16),
            "tensor",
            scatter_dimension=0,
            tiled=True,
        ).astype(jnp.float32)
        block_out = (middle + mlp_branch + proj_bias).astype(jnp.bfloat16)
        grad_proj = jnp.einsum(
            "lbo,lbf->of", grad_top_full, activated, preferred_element_type=jnp.float32
        )
        grad_act = jnp.einsum(
            "lbo,of->lbf", grad_top_full, proj_full, preferred_element_type=jnp.float32
        )
        _, gelu_pull = jax.vjp(gelu_tanh, pre_act)
        grad_pre = gelu_pull(grad_act)[0].astype(jnp.bfloat16)
        grad_fc_bias = jnp.sum(grad_pre.astype(jnp.float32), axis=(0, 1))
        grad_fc = jnp.einsum(
            "lbd,lbf->df", hidden2_full, grad_pre, preferred_element_type=jnp.float32
        )
        grad_h2 = lax.psum_scatter(
            jnp.einsum("lbf,df->lbd", grad_pre, fc_full, preferred_element_type=jnp.float32),
            "tensor",
            scatter_dimension=0,
            tiled=True,
        )
        grad_gain2 = jnp.sum(grad_h2 * normed2, axis=(0, 1))
        grad_shift2 = jnp.sum(grad_h2, axis=(0, 1))
        grad_mid = grad_top.astype(jnp.float32) + norm_back(grad_h2, normed2, inverse2, norm2_gain)
        grad_out_bias = jnp.sum(grad_mid, axis=(0, 1))
        grad_proj_bias = jnp.sum(grad_top.astype(jnp.float32), axis=(0, 1))
        grad_mid_full = lax.all_gather(grad_mid.astype(jnp.bfloat16), "tensor", axis=0, tiled=True)
        grad_out_w = jnp.einsum(
            "lbo,lbi->oi", grad_mid_full, mixed, preferred_element_type=jnp.float32
        )
        grad_mixed = jnp.einsum(
            "lbo,oi->lbi", grad_mid_full, out_full, preferred_element_type=jnp.float32
        )
        grad_mixed = grad_mixed.astype(jnp.bfloat16).reshape(length, batch, heads_local, HEAD_DIM)
        grad_queries, grad_keys, grad_values = attend_backward(
            queries, keys, values, log_totals, grad_mixed
        )
        grad_qkv = jnp.stack([grad_queries, grad_keys, grad_values], axis=2).astype(jnp.bfloat16)
        grad_qkv = grad_qkv.reshape(length, batch, 3, heads_local * HEAD_DIM)
        kind_sums = jnp.sum(grad_qkv.astype(jnp.float32), axis=(0, 1))
        grad_qv_bias = jnp.stack([kind_sums[0], kind_sums[2]])
        grad_qkv_w = jnp.einsum(
            "lbd,lbce->dce", hidden1_full, grad_qkv, preferred_element_type=jnp.float32
        )
        grad_h1 = lax.psum_scatter(
            jnp.einsum("lbce,dce->lbd", grad_qkv, qkv_full, preferred_element_type=jnp.float32),
            "tensor",
            scatter_dimension=0,
            tiled=True,
        )
        grad_gain1 = jnp.sum(grad_h1 * normed1, axis=(0, 1))
        grad_shift1 = jnp.sum(grad_h1, axis=(0, 1))
        grad_in = (grad_mid + norm_back(grad_h1, normed1, inverse1, norm1_gain)).astype(
            jnp.bfloat16
        )
        fresh_weights = jnp.concatenate(
            [grad_qkv_w.reshape(depth, width_qkv), grad_out_w, grad_fc, grad_proj], axis=1
        )
        weight_acc = weight_acc + fresh_weights
        fresh = (
            grad_qv_bias,
            grad_fc_bias,
            grad_out_bias,
            grad_proj_bias,
            grad_gain1,
            grad_shift1,
            grad_gain2,
            grad_shift2,
        )
        small_acc = tuple((total + extra for total, extra in zip(small_acc, fresh)))
        outputs_all = lax.dynamic_update_index_in_dim(outputs_all, block_out, index, 0)
        in_grads_all = lax.dynamic_update_index_in_dim(in_grads_all, grad_in, index, 0)
        return (outputs_all, in_grads_all, weight_acc, small_acc)

    outputs_all, in_grads_all, weight_acc, small_acc = lax.fori_loop(
        0, micro, one_micro, (outputs_init, in_grads_init, weight_init, small_init)
    )
    weight_shard = lax.psum_scatter(weight_acc, "dp", scatter_dimension=0, tiled=True)
    grad_qkv_w = weight_shard[:, : cuts[0]].reshape(qkv_weight.shape)
    grad_out_w = weight_shard[:, cuts[0] : cuts[1]]
    grad_fc_w = weight_shard[:, cuts[1] : cuts[2]]
    grad_proj_w = weight_shard[:, cuts[2] :]
    tensor_size = lax.psum(1, "tensor")
    slot = lax.axis_index("tensor")
    head_vec = jnp.concatenate([small_acc[0].reshape(-1), small_acc[1]])
    head_slots = jnp.zeros((tensor_size, head_vec.shape[0]), jnp.float32)
    head_slots = lax.dynamic_update_index_in_dim(head_slots, head_vec, slot, 0)
    feature_vec = jnp.concatenate([item for item in small_acc[2:]])
    total = lax.psum(jnp.concatenate([feature_vec, head_slots.reshape(-1)]), ("dp", "tensor"))
    features = total[: feature_vec.shape[0]].reshape(6, -1)
    head_total = lax.dynamic_index_in_dim(
        total[feature_vec.shape[0] :].reshape(tensor_size, -1), slot, 0, keepdims=False
    )
    qv_size = small_acc[0].size
    grad_qv_bias = head_total[:qv_size].reshape(small_acc[0].shape)
    grad_fc_bias = head_total[qv_size:]
    return (
        outputs_all,
        in_grads_all,
        grad_qkv_w,
        grad_qv_bias,
        grad_out_w,
        features[0],
        grad_fc_w,
        grad_fc_bias,
        grad_proj_w,
        features[1],
        features[2],
        features[3],
        features[4],
        features[5],
    )


def solution(mesh):
    in_specs = (
        P(None, "tensor", "dp", None),
        P("dp", None, "tensor"),
        P(None, "tensor"),
        P("dp", "tensor"),
        P(),
        P("dp", "tensor"),
        P("tensor"),
        P("dp", "tensor"),
        P(),
        P(),
        P(),
        P(),
        P(),
        P(None, "tensor", "dp", None),
    )
    out_specs = (
        P(None, "tensor", "dp", None),
        P(None, "tensor", "dp", None),
        P("dp", None, "tensor"),
        P(None, "tensor"),
        P("dp", "tensor"),
        P(),
        P("dp", "tensor"),
        P("tensor"),
        P("dp", "tensor"),
        P(),
        P(),
        P(),
        P(),
        P(),
    )
    return jax.shard_map(
        per_device, mesh=mesh, in_specs=in_specs, out_specs=out_specs, check_vma=False
    )
```

```python
import jax
import jax.numpy as jnp
from jax import lax
from jax.sharding import PartitionSpec as P

HEAD_DIM = 64


norm_eps = 1e-05
tanh_coef = 0.7978845608028654
cube_coef = 0.044715
block_rows = 512


def gelu_tanh(values):
    return (
        0.5 * values * (1.0 + jnp.tanh(tanh_coef * (values + cube_coef * values * values * values)))
    )


def norm_parts(rows):
    center = rows - jnp.mean(rows, axis=-1, keepdims=True)
    spread = jnp.mean(center * center, axis=-1, keepdims=True)
    inverse = lax.rsqrt(spread + norm_eps)
    return (center * inverse, inverse)


def norm_back(grad_out, normed, inverse, gain):
    grad_normed = grad_out * gain
    first = jnp.mean(grad_normed, axis=-1, keepdims=True)
    second = jnp.mean(grad_normed * normed, axis=-1, keepdims=True)
    return inverse * (grad_normed - first - normed * second)


def causal_scores(query_block, keys, offset):
    scores = jnp.einsum(
        "qbhe,kbhe->bhqk", query_block, keys, preferred_element_type=jnp.float32
    ) * HEAD_DIM ** (-0.5)
    height = query_block.shape[0]
    length = keys.shape[0]
    row_pos = lax.broadcasted_iota(jnp.int32, (height, length), 0) + offset
    col_pos = lax.broadcasted_iota(jnp.int32, (height, length), 1)
    return jnp.where(col_pos <= row_pos, scores, -1e30)


def attend_forward(queries, keys, values):
    length = keys.shape[0]
    span = min(block_rows, length)
    outputs = []
    totals = []
    for offset in range(0, length, span):
        scores = causal_scores(queries[offset : offset + span], keys, offset)
        peak = jnp.max(scores, axis=-1, keepdims=True)
        raised = jnp.exp(scores - peak)
        total = jnp.sum(raised, axis=-1, keepdims=True)
        weights = (raised / total).astype(jnp.bfloat16)
        outputs.append(
            jnp.einsum("bhqk,kbhe->qbhe", weights, values, preferred_element_type=jnp.float32)
        )
        totals.append(peak + jnp.log(total))
    return (jnp.concatenate(outputs, 0), jnp.concatenate(totals, 2))


def attend_backward(queries, keys, values, log_totals, grad_out):
    length = keys.shape[0]
    span = min(block_rows, length)
    scale = HEAD_DIM ** (-0.5)
    grad_queries = []
    grad_keys = jnp.zeros(keys.shape, jnp.float32)
    grad_values = jnp.zeros(values.shape, jnp.float32)
    for offset in range(0, length, span):
        query_block = queries[offset : offset + span]
        grad_block = grad_out[offset : offset + span]
        scores = causal_scores(query_block, keys, offset)
        probs = jnp.exp(scores - log_totals[:, :, offset : offset + span])
        grad_probs = jnp.einsum(
            "qbhe,kbhe->bhqk", grad_block, values, preferred_element_type=jnp.float32
        )
        inner = jnp.sum(probs * grad_probs, axis=-1, keepdims=True)
        grad_scores = (probs * (grad_probs - inner)).astype(jnp.bfloat16)
        grad_queries.append(
            jnp.einsum("bhqk,kbhe->qbhe", grad_scores, keys, preferred_element_type=jnp.float32)
            * scale
        )
        grad_keys = (
            grad_keys
            + jnp.einsum(
                "bhqk,qbhe->kbhe", grad_scores, query_block, preferred_element_type=jnp.float32
            )
            * scale
        )
        grad_values = grad_values + jnp.einsum(
            "bhqk,qbhe->kbhe",
            probs.astype(jnp.bfloat16),
            grad_block,
            preferred_element_type=jnp.float32,
        )
    return (jnp.concatenate(grad_queries, 0), grad_keys, grad_values)


SWAP = [(0, 1), (1, 0)]


def tensor_gather(block):
    across = lax.axis_index("tx")
    core = lax.axis_index("tc")
    other = lax.ppermute(block, "tx", SWAP)
    pair = jnp.where(across == 0, jnp.stack([block, other]), jnp.stack([other, block]))
    pair_other = lax.ppermute(pair, "tc", SWAP)
    full = jnp.where(
        core == 0, jnp.stack([pair, pair_other], 1), jnp.stack([pair_other, pair], 1)
    )
    return full.reshape((4 * block.shape[0],) + block.shape[1:])


def tensor_scatter(parts, send_dtype):
    across = lax.axis_index("tx")
    core = lax.axis_index("tc")
    rows = parts.shape[0] // 4
    grid = parts.reshape((2, 2, rows) + parts.shape[1:])
    keep = lax.dynamic_index_in_dim(grid, core, 1, keepdims=False)
    send = lax.dynamic_index_in_dim(grid, 1 - core, 1, keepdims=False)
    got = lax.ppermute(send.astype(send_dtype), "tc", SWAP)
    chip = keep + got.astype(jnp.float32)
    keep2 = lax.dynamic_index_in_dim(chip, across, 0, keepdims=False)
    send2 = lax.dynamic_index_in_dim(chip, 1 - across, 0, keepdims=False)
    got2 = lax.ppermute(send2.astype(send_dtype), "tx", SWAP)
    return keep2 + got2.astype(jnp.float32)


def per_device(
    block_input,
    qkv_weight,
    qv_bias,
    out_weight,
    out_bias,
    fc_weight,
    fc_bias,
    proj_weight,
    proj_bias,
    norm1_gain,
    norm1_shift,
    norm2_gain,
    norm2_shift,
    out_grad,
):
    micro = block_input.shape[0]
    heads_local = qkv_weight.shape[2] // HEAD_DIM
    rows = qkv_weight.shape[0]
    width_qkv = qkv_weight.shape[1] * qkv_weight.shape[2]
    width_out = out_weight.shape[1]
    width_fc = fc_weight.shape[1]
    cuts = (width_qkv, width_qkv + width_out, width_qkv + width_out + width_fc)
    packed = jnp.concatenate(
        [qkv_weight.reshape(rows, width_qkv), out_weight, fc_weight, proj_weight], axis=1
    )
    packed_full = lax.all_gather(packed, "dp", axis=0, tiled=True)
    depth = packed_full.shape[0]
    qkv_full = packed_full[:, : cuts[0]].reshape(depth, 3, qkv_weight.shape[2])
    out_full = packed_full[:, cuts[0] : cuts[1]]
    fc_full = packed_full[:, cuts[1] : cuts[2]]
    proj_full = packed_full[:, cuts[2] :]
    grad_top_all = jnp.swapaxes(tensor_gather(jnp.swapaxes(out_grad, 0, 1)), 0, 1)
    weight_init = jnp.zeros(packed_full.shape, jnp.float32)
    small_init = (
        jnp.zeros(qv_bias.shape, jnp.float32),
        jnp.zeros(fc_bias.shape, jnp.float32),
        jnp.zeros(out_bias.shape, jnp.float32),
        jnp.zeros(proj_bias.shape, jnp.float32),
        jnp.zeros(norm1_gain.shape, jnp.float32),
        jnp.zeros(norm1_shift.shape, jnp.float32),
        jnp.zeros(norm2_gain.shape, jnp.float32),
        jnp.zeros(norm2_shift.shape, jnp.float32),
    )
    outputs_init = jnp.zeros(block_input.shape, jnp.bfloat16)
    in_grads_init = jnp.zeros(block_input.shape, jnp.bfloat16)

    def one_micro(index, carry):
        outputs_all, in_grads_all, weight_acc, small_acc = carry
        resid_in = lax.dynamic_index_in_dim(block_input, index, 0, keepdims=False).astype(
            jnp.float32
        )
        grad_top = lax.dynamic_index_in_dim(out_grad, index, 0, keepdims=False)
        grad_top_full = lax.dynamic_index_in_dim(grad_top_all, index, 0, keepdims=False)
        normed1, inverse1 = norm_parts(resid_in)
        hidden1 = (normed1 * norm1_gain + norm1_shift).astype(jnp.bfloat16)
        hidden1_full = tensor_gather(hidden1)
        length = hidden1_full.shape[0]
        batch = hidden1_full.shape[1]
        projected = jnp.einsum(
            "lbd,dce->lbce", hidden1_full, qkv_full, preferred_element_type=jnp.float32
        )
        qkv_bias = jnp.stack([qv_bias[0], jnp.zeros_like(qv_bias[0]), qv_bias[1]])
        qkv_values = (projected + qkv_bias).astype(jnp.bfloat16)
        split = qkv_values.reshape(length, batch, 3, heads_local, HEAD_DIM)
        queries = split[:, :, 0]
        keys = split[:, :, 1]
        values = split[:, :, 2]
        attended, log_totals = attend_forward(queries, keys, values)
        mixed = attended.astype(jnp.bfloat16).reshape(length, batch, heads_local * HEAD_DIM)
        attn_branch = tensor_scatter(
            jnp.einsum("lbi,oi->lbo", mixed, out_full, preferred_element_type=jnp.float32),
            jnp.float32,
        )
        middle = resid_in + attn_branch + out_bias
        normed2, inverse2 = norm_parts(middle)
        hidden2 = (normed2 * norm2_gain + norm2_shift).astype(jnp.bfloat16)
        hidden2_full = tensor_gather(hidden2)
        pre_act = (
            jnp.einsum("lbd,df->lbf", hidden2_full, fc_full, preferred_element_type=jnp.float32)
            + fc_bias
        )
        activated = gelu_tanh(pre_act).astype(jnp.bfloat16)
        mlp_branch = tensor_scatter(
            jnp.einsum("lbf,of->lbo", activated, proj_full, preferred_element_type=jnp.float32),
            jnp.bfloat16,
        )
        block_out = (middle + mlp_branch + proj_bias).astype(jnp.bfloat16)
        grad_proj = jnp.einsum(
            "lbo,lbf->of", grad_top_full, activated, preferred_element_type=jnp.float32
        )
        grad_act = jnp.einsum(
            "lbo,of->lbf", grad_top_full, proj_full, preferred_element_type=jnp.float32
        )
        _, gelu_pull = jax.vjp(gelu_tanh, pre_act)
        grad_pre = gelu_pull(grad_act)[0].astype(jnp.bfloat16)
        grad_fc_bias = jnp.sum(grad_pre.astype(jnp.float32), axis=(0, 1))
        grad_fc = jnp.einsum(
            "lbd,lbf->df", hidden2_full, grad_pre, preferred_element_type=jnp.float32
        )
        grad_h2 = tensor_scatter(
            jnp.einsum("lbf,df->lbd", grad_pre, fc_full, preferred_element_type=jnp.float32),
            jnp.float32,
        )
        grad_gain2 = jnp.sum(grad_h2 * normed2, axis=(0, 1))
        grad_shift2 = jnp.sum(grad_h2, axis=(0, 1))
        grad_mid = grad_top.astype(jnp.float32) + norm_back(grad_h2, normed2, inverse2, norm2_gain)
        grad_out_bias = jnp.sum(grad_mid, axis=(0, 1))
        grad_proj_bias = jnp.sum(grad_top.astype(jnp.float32), axis=(0, 1))
        grad_mid_full = tensor_gather(grad_mid.astype(jnp.bfloat16))
        grad_out_w = jnp.einsum(
            "lbo,lbi->oi", grad_mid_full, mixed, preferred_element_type=jnp.float32
        )
        grad_mixed = jnp.einsum(
            "lbo,oi->lbi", grad_mid_full, out_full, preferred_element_type=jnp.float32
        )
        grad_mixed = grad_mixed.astype(jnp.bfloat16).reshape(length, batch, heads_local, HEAD_DIM)
        grad_queries, grad_keys, grad_values = attend_backward(
            queries, keys, values, log_totals, grad_mixed
        )
        grad_qkv = jnp.stack([grad_queries, grad_keys, grad_values], axis=2).astype(jnp.bfloat16)
        grad_qkv = grad_qkv.reshape(length, batch, 3, heads_local * HEAD_DIM)
        kind_sums = jnp.sum(grad_qkv.astype(jnp.float32), axis=(0, 1))
        grad_qv_bias = jnp.stack([kind_sums[0], kind_sums[2]])
        grad_qkv_w = jnp.einsum(
            "lbd,lbce->dce", hidden1_full, grad_qkv, preferred_element_type=jnp.float32
        )
        grad_h1 = tensor_scatter(
            jnp.einsum("lbce,dce->lbd", grad_qkv, qkv_full, preferred_element_type=jnp.float32),
            jnp.float32,
        )
        grad_gain1 = jnp.sum(grad_h1 * normed1, axis=(0, 1))
        grad_shift1 = jnp.sum(grad_h1, axis=(0, 1))
        grad_in = (grad_mid + norm_back(grad_h1, normed1, inverse1, norm1_gain)).astype(
            jnp.bfloat16
        )
        fresh_weights = jnp.concatenate(
            [grad_qkv_w.reshape(depth, width_qkv), grad_out_w, grad_fc, grad_proj], axis=1
        )
        weight_acc = weight_acc + fresh_weights
        fresh = (
            grad_qv_bias,
            grad_fc_bias,
            grad_out_bias,
            grad_proj_bias,
            grad_gain1,
            grad_shift1,
            grad_gain2,
            grad_shift2,
        )
        small_acc = tuple((total + extra for total, extra in zip(small_acc, fresh)))
        outputs_all = lax.dynamic_update_index_in_dim(outputs_all, block_out, index, 0)
        in_grads_all = lax.dynamic_update_index_in_dim(in_grads_all, grad_in, index, 0)
        return (outputs_all, in_grads_all, weight_acc, small_acc)

    outputs_all, in_grads_all, weight_acc, small_acc = lax.fori_loop(
        0, micro, one_micro, (outputs_init, in_grads_init, weight_init, small_init)
    )
    weight_shard = lax.psum_scatter(weight_acc, "dp", scatter_dimension=0, tiled=True)
    grad_qkv_w = weight_shard[:, : cuts[0]].reshape(qkv_weight.shape)
    grad_out_w = weight_shard[:, cuts[0] : cuts[1]]
    grad_fc_w = weight_shard[:, cuts[1] : cuts[2]]
    grad_proj_w = weight_shard[:, cuts[2] :]
    tensor_size = 4
    slot = lax.axis_index("tx") * 2 + lax.axis_index("tc")
    head_vec = jnp.concatenate([small_acc[0].reshape(-1), small_acc[1]])
    head_slots = jnp.zeros((tensor_size, head_vec.shape[0]), jnp.float32)
    head_slots = lax.dynamic_update_index_in_dim(head_slots, head_vec, slot, 0)
    feature_vec = jnp.concatenate([item for item in small_acc[2:]])
    total = lax.psum(jnp.concatenate([feature_vec, head_slots.reshape(-1)]), ("dp", "tx", "tc"))
    features = total[: feature_vec.shape[0]].reshape(6, -1)
    head_total = lax.dynamic_index_in_dim(
        total[feature_vec.shape[0] :].reshape(tensor_size, -1), slot, 0, keepdims=False
    )
    qv_size = small_acc[0].size
    grad_qv_bias = head_total[:qv_size].reshape(small_acc[0].shape)
    grad_fc_bias = head_total[qv_size:]
    return (
        outputs_all,
        in_grads_all,
        grad_qkv_w,
        grad_qv_bias,
        grad_out_w,
        features[0],
        grad_fc_w,
        grad_fc_bias,
        grad_proj_w,
        features[1],
        features[2],
        features[3],
        features[4],
        features[5],
    )


def solution(mesh):
    assert mesh.shape["tensor"] == 4
    devices = mesh.devices.reshape(mesh.shape["dp"], 2, 2)
    mesh = jax.sharding.Mesh(devices, ("dp", "tx", "tc"))
    in_specs = (
        P(None, ("tx", "tc"), "dp", None),
        P("dp", None, ("tx", "tc")),
        P(None, ("tx", "tc")),
        P("dp", ("tx", "tc")),
        P(),
        P("dp", ("tx", "tc")),
        P(("tx", "tc")),
        P("dp", ("tx", "tc")),
        P(),
        P(),
        P(),
        P(),
        P(),
        P(None, ("tx", "tc"), "dp", None),
    )
    out_specs = (
        P(None, ("tx", "tc"), "dp", None),
        P(None, ("tx", "tc"), "dp", None),
        P("dp", None, ("tx", "tc")),
        P(None, ("tx", "tc")),
        P("dp", ("tx", "tc")),
        P(),
        P("dp", ("tx", "tc")),
        P(("tx", "tc")),
        P("dp", ("tx", "tc")),
        P(),
        P(),
        P(),
        P(),
        P(),
    )
    return jax.shard_map(
        per_device, mesh=mesh, in_specs=in_specs, out_specs=out_specs, check_vma=False
    )
```

```python
import jax
import jax.numpy as jnp
from jax import lax
from jax.sharding import PartitionSpec as P

HEAD_DIM = 64


norm_eps = 1e-05
tanh_coef = 0.7978845608028654
cube_coef = 0.044715
block_rows = 512


def gelu_tanh(values):
    return (
        0.5 * values * (1.0 + jnp.tanh(tanh_coef * (values + cube_coef * values * values * values)))
    )


def norm_parts(rows):
    center = rows - jnp.mean(rows, axis=-1, keepdims=True)
    spread = jnp.mean(center * center, axis=-1, keepdims=True)
    inverse = lax.rsqrt(spread + norm_eps)
    return (center * inverse, inverse)


def norm_back(grad_out, normed, inverse, gain):
    grad_normed = grad_out * gain
    first = jnp.mean(grad_normed, axis=-1, keepdims=True)
    second = jnp.mean(grad_normed * normed, axis=-1, keepdims=True)
    return inverse * (grad_normed - first - normed * second)


def causal_scores(query_block, keys, offset):
    scores = jnp.einsum(
        "qbhe,kbhe->bhqk", query_block, keys, preferred_element_type=jnp.float32
    ) * HEAD_DIM ** (-0.5)
    height = query_block.shape[0]
    length = keys.shape[0]
    row_pos = lax.broadcasted_iota(jnp.int32, (height, length), 0) + offset
    col_pos = lax.broadcasted_iota(jnp.int32, (height, length), 1)
    return jnp.where(col_pos <= row_pos, scores, -1e30)


def attend_forward(queries, keys, values):
    length = keys.shape[0]
    span = min(block_rows, length)
    outputs = []
    totals = []
    for offset in range(0, length, span):
        scores = causal_scores(queries[offset : offset + span], keys, offset)
        peak = jnp.max(scores, axis=-1, keepdims=True)
        raised = jnp.exp(scores - peak)
        total = jnp.sum(raised, axis=-1, keepdims=True)
        weights = (raised / total).astype(jnp.bfloat16)
        outputs.append(
            jnp.einsum("bhqk,kbhe->qbhe", weights, values, preferred_element_type=jnp.float32)
        )
        totals.append(peak + jnp.log(total))
    return (jnp.concatenate(outputs, 0), jnp.concatenate(totals, 2))


def attend_backward(queries, keys, values, log_totals, grad_out):
    length = keys.shape[0]
    span = min(block_rows, length)
    scale = HEAD_DIM ** (-0.5)
    grad_queries = []
    grad_keys = jnp.zeros(keys.shape, jnp.float32)
    grad_values = jnp.zeros(values.shape, jnp.float32)
    for offset in range(0, length, span):
        query_block = queries[offset : offset + span]
        grad_block = grad_out[offset : offset + span]
        scores = causal_scores(query_block, keys, offset)
        probs = jnp.exp(scores - log_totals[:, :, offset : offset + span])
        grad_probs = jnp.einsum(
            "qbhe,kbhe->bhqk", grad_block, values, preferred_element_type=jnp.float32
        )
        inner = jnp.sum(probs * grad_probs, axis=-1, keepdims=True)
        grad_scores = (probs * (grad_probs - inner)).astype(jnp.bfloat16)
        grad_queries.append(
            jnp.einsum("bhqk,kbhe->qbhe", grad_scores, keys, preferred_element_type=jnp.float32)
            * scale
        )
        grad_keys = (
            grad_keys
            + jnp.einsum(
                "bhqk,qbhe->kbhe", grad_scores, query_block, preferred_element_type=jnp.float32
            )
            * scale
        )
        grad_values = grad_values + jnp.einsum(
            "bhqk,qbhe->kbhe",
            probs.astype(jnp.bfloat16),
            grad_block,
            preferred_element_type=jnp.float32,
        )
    return (jnp.concatenate(grad_queries, 0), grad_keys, grad_values)


SWAP = [(0, 1), (1, 0)]


def tensor_gather(block):
    across = lax.axis_index("tx")
    core = lax.axis_index("tc")
    other = lax.ppermute(block, "tx", SWAP)
    pair = jnp.where(across == 0, jnp.stack([block, other]), jnp.stack([other, block]))
    pair_other = lax.ppermute(pair, "tc", SWAP)
    full = jnp.where(
        core == 0, jnp.stack([pair, pair_other], 1), jnp.stack([pair_other, pair], 1)
    )
    return full.reshape((4 * block.shape[0],) + block.shape[1:])


def tensor_scatter(parts, send_dtype):
    across = lax.axis_index("tx")
    core = lax.axis_index("tc")
    rows = parts.shape[0] // 4
    grid = parts.reshape((2, 2, rows) + parts.shape[1:])
    keep = lax.dynamic_index_in_dim(grid, core, 1, keepdims=False)
    send = lax.dynamic_index_in_dim(grid, 1 - core, 1, keepdims=False)
    got = lax.ppermute(send.astype(send_dtype), "tc", SWAP)
    chip = keep + got.astype(jnp.float32)
    keep2 = lax.dynamic_index_in_dim(chip, across, 0, keepdims=False)
    send2 = lax.dynamic_index_in_dim(chip, 1 - across, 0, keepdims=False)
    got2 = lax.ppermute(send2.astype(send_dtype), "tx", SWAP)
    return keep2 + got2.astype(jnp.float32)


def tensor_sum(vector):
    vector = vector + lax.ppermute(vector, "tc", SWAP)
    return vector + lax.ppermute(vector, "tx", SWAP)


def one_micro(resid_in, grad_top, grad_top_full, weights, params):
    qkv_full, out_full, fc_full, proj_full = weights
    qv_bias, out_bias, fc_bias, proj_bias, norm1_gain, norm1_shift, norm2_gain, norm2_shift = params
    heads_local = qkv_full.shape[2] // HEAD_DIM
    normed1, inverse1 = norm_parts(resid_in)
    hidden1 = (normed1 * norm1_gain + norm1_shift).astype(jnp.bfloat16)
    hidden1_full = tensor_gather(hidden1)
    length = hidden1_full.shape[0]
    batch = hidden1_full.shape[1]
    projected = jnp.einsum(
        "lbd,dce->lbce", hidden1_full, qkv_full, preferred_element_type=jnp.float32
    )
    qkv_bias = jnp.stack([qv_bias[0], jnp.zeros_like(qv_bias[0]), qv_bias[1]])
    qkv_values = (projected + qkv_bias).astype(jnp.bfloat16)
    split = qkv_values.reshape(length, batch, 3, heads_local, HEAD_DIM)
    queries = split[:, :, 0]
    keys = split[:, :, 1]
    values = split[:, :, 2]
    attended, log_totals = attend_forward(queries, keys, values)
    mixed = attended.astype(jnp.bfloat16).reshape(length, batch, heads_local * HEAD_DIM)
    attn_branch = tensor_scatter(
        jnp.einsum("lbi,oi->lbo", mixed, out_full, preferred_element_type=jnp.float32),
        jnp.float32,
    )
    middle = resid_in + attn_branch + out_bias
    normed2, inverse2 = norm_parts(middle)
    hidden2 = (normed2 * norm2_gain + norm2_shift).astype(jnp.bfloat16)
    hidden2_full = tensor_gather(hidden2)
    pre_act = (
        jnp.einsum("lbd,df->lbf", hidden2_full, fc_full, preferred_element_type=jnp.float32)
        + fc_bias
    )
    activated = gelu_tanh(pre_act).astype(jnp.bfloat16)
    mlp_branch = tensor_scatter(
        jnp.einsum("lbf,of->lbo", activated, proj_full, preferred_element_type=jnp.float32),
        jnp.bfloat16,
    )
    block_out = (middle + mlp_branch + proj_bias).astype(jnp.bfloat16)
    grad_proj = jnp.einsum(
        "lbo,lbf->of", grad_top_full, activated, preferred_element_type=jnp.float32
    )
    grad_act = jnp.einsum(
        "lbo,of->lbf", grad_top_full, proj_full, preferred_element_type=jnp.float32
    )
    _, gelu_pull = jax.vjp(gelu_tanh, pre_act)
    grad_pre = gelu_pull(grad_act)[0].astype(jnp.bfloat16)
    grad_fc_bias = jnp.sum(grad_pre.astype(jnp.float32), axis=(0, 1))
    grad_fc = jnp.einsum(
        "lbd,lbf->df", hidden2_full, grad_pre, preferred_element_type=jnp.float32
    )
    grad_h2 = tensor_scatter(
        jnp.einsum("lbf,df->lbd", grad_pre, fc_full, preferred_element_type=jnp.float32),
        jnp.float32,
    )
    grad_gain2 = jnp.sum(grad_h2 * normed2, axis=(0, 1))
    grad_shift2 = jnp.sum(grad_h2, axis=(0, 1))
    grad_mid = grad_top.astype(jnp.float32) + norm_back(grad_h2, normed2, inverse2, norm2_gain)
    grad_out_bias = jnp.sum(grad_mid, axis=(0, 1))
    grad_proj_bias = jnp.sum(grad_top.astype(jnp.float32), axis=(0, 1))
    grad_mid_full = tensor_gather(grad_mid.astype(jnp.bfloat16))
    grad_out_w = jnp.einsum(
        "lbo,lbi->oi", grad_mid_full, mixed, preferred_element_type=jnp.float32
    )
    grad_mixed = jnp.einsum(
        "lbo,oi->lbi", grad_mid_full, out_full, preferred_element_type=jnp.float32
    )
    grad_mixed = grad_mixed.astype(jnp.bfloat16).reshape(length, batch, heads_local, HEAD_DIM)
    grad_queries, grad_keys, grad_values = attend_backward(
        queries, keys, values, log_totals, grad_mixed
    )
    grad_qkv = jnp.stack([grad_queries, grad_keys, grad_values], axis=2).astype(jnp.bfloat16)
    grad_qkv = grad_qkv.reshape(length, batch, 3, heads_local * HEAD_DIM)
    kind_sums = jnp.sum(grad_qkv.astype(jnp.float32), axis=(0, 1))
    grad_qv_bias = jnp.stack([kind_sums[0], kind_sums[2]])
    grad_qkv_w = jnp.einsum(
        "lbd,lbce->dce", hidden1_full, grad_qkv, preferred_element_type=jnp.float32
    )
    grad_h1 = tensor_scatter(
        jnp.einsum("lbce,dce->lbd", grad_qkv, qkv_full, preferred_element_type=jnp.float32),
        jnp.float32,
    )
    grad_gain1 = jnp.sum(grad_h1 * normed1, axis=(0, 1))
    grad_shift1 = jnp.sum(grad_h1, axis=(0, 1))
    grad_in = (grad_mid + norm_back(grad_h1, normed1, inverse1, norm1_gain)).astype(
        jnp.bfloat16
    )
    depth = qkv_full.shape[0]
    mlp_grads = jnp.concatenate([grad_fc, grad_proj], axis=1)
    attn_grads = jnp.concatenate([grad_qkv_w.reshape(depth, -1), grad_out_w], axis=1)
    head_sums = jnp.concatenate([grad_qv_bias.reshape(-1), grad_fc_bias])
    feature_sums = jnp.concatenate(
        [grad_out_bias, grad_proj_bias, grad_gain1, grad_shift1, grad_gain2, grad_shift2]
    )
    return block_out, grad_in, mlp_grads, attn_grads, head_sums, feature_sums


def per_device(
    block_input,
    qkv_weight,
    qv_bias,
    out_weight,
    out_bias,
    fc_weight,
    fc_bias,
    proj_weight,
    proj_bias,
    norm1_gain,
    norm1_shift,
    norm2_gain,
    norm2_shift,
    out_grad,
):
    micro = block_input.shape[0]
    rows = qkv_weight.shape[0]
    width_qkv = qkv_weight.shape[1] * qkv_weight.shape[2]
    width_fc = fc_weight.shape[1]
    attn_pack = jnp.concatenate([qkv_weight.reshape(rows, width_qkv), out_weight], axis=1)
    mlp_pack = jnp.concatenate([fc_weight, proj_weight], axis=1)
    attn_full = lax.all_gather(attn_pack, "dp", axis=0, tiled=True)
    mlp_full = lax.all_gather(mlp_pack, "dp", axis=0, tiled=True)
    depth = attn_full.shape[0]
    weights = (
        attn_full[:, :width_qkv].reshape(depth, 3, qkv_weight.shape[2]),
        attn_full[:, width_qkv:],
        mlp_full[:, :width_fc],
        mlp_full[:, width_fc:],
    )
    params = (qv_bias, out_bias, fc_bias, proj_bias, norm1_gain, norm1_shift, norm2_gain, norm2_shift)
    grad_top_all = jnp.swapaxes(tensor_gather(jnp.swapaxes(out_grad, 0, 1)), 0, 1)
    outputs, in_grads = [], []
    mlp_acc = attn_acc = head_acc = feature_acc = None
    for index in range(micro):
        block_out, grad_in, mlp_grads, attn_grads, head_sums, feature_sums = one_micro(
            block_input[index].astype(jnp.float32),
            out_grad[index],
            grad_top_all[index],
            weights,
            params,
        )
        outputs.append(block_out)
        in_grads.append(grad_in)
        if index == 0:
            mlp_acc, attn_acc, head_acc, feature_acc = mlp_grads, attn_grads, head_sums, feature_sums
        else:
            mlp_acc = mlp_acc + mlp_grads
            attn_acc = attn_acc + attn_grads
            head_acc = head_acc + head_sums
            feature_acc = feature_acc + feature_sums
    mlp_shard = lax.psum_scatter(mlp_acc, "dp", scatter_dimension=0, tiled=True)
    small = jnp.concatenate([tensor_sum(feature_acc), head_acc])
    width_attn = attn_acc.shape[1]
    small_rows = -(-small.shape[0] // width_attn)
    small = jnp.pad(small, (0, small_rows * width_attn - small.shape[0])).reshape(
        small_rows, width_attn
    )
    blocks = depth // rows
    attn_rows = jnp.concatenate(
        [
            attn_acc.reshape(blocks, rows, width_attn),
            jnp.broadcast_to(small, (blocks, small_rows, width_attn)),
        ],
        axis=1,
    ).reshape(blocks * (rows + small_rows), width_attn)
    attn_shard = lax.psum_scatter(attn_rows, "dp", scatter_dimension=0, tiled=True)
    small_total = attn_shard[rows:].reshape(-1)
    features = small_total[: feature_acc.shape[0]].reshape(6, -1)
    head_total = small_total[feature_acc.shape[0] : feature_acc.shape[0] + head_acc.shape[0]]
    qv_size = qv_bias.size
    return (
        jnp.stack(outputs),
        jnp.stack(in_grads),
        attn_shard[:rows, :width_qkv].reshape(qkv_weight.shape),
        head_total[:qv_size].reshape(qv_bias.shape),
        attn_shard[:rows, width_qkv:],
        features[0],
        mlp_shard[:, :width_fc],
        head_total[qv_size:],
        mlp_shard[:, width_fc:],
        features[1],
        features[2],
        features[3],
        features[4],
        features[5],
    )


def solution(mesh):
    assert mesh.shape["tensor"] == 4
    devices = mesh.devices.reshape(mesh.shape["dp"], 2, 2)
    mesh = jax.sharding.Mesh(devices, ("dp", "tx", "tc"))
    in_specs = (
        P(None, ("tx", "tc"), "dp", None),
        P("dp", None, ("tx", "tc")),
        P(None, ("tx", "tc")),
        P("dp", ("tx", "tc")),
        P(),
        P("dp", ("tx", "tc")),
        P(("tx", "tc")),
        P("dp", ("tx", "tc")),
        P(),
        P(),
        P(),
        P(),
        P(),
        P(None, ("tx", "tc"), "dp", None),
    )
    out_specs = (
        P(None, ("tx", "tc"), "dp", None),
        P(None, ("tx", "tc"), "dp", None),
        P("dp", None, ("tx", "tc")),
        P(None, ("tx", "tc")),
        P("dp", ("tx", "tc")),
        P(),
        P("dp", ("tx", "tc")),
        P(("tx", "tc")),
        P("dp", ("tx", "tc")),
        P(),
        P(),
        P(),
        P(),
        P(),
    )
    return jax.shard_map(
        per_device, mesh=mesh, in_specs=in_specs, out_specs=out_specs, check_vma=False
    )
```

```python
import jax
import jax.numpy as jnp
from jax import lax
from jax.sharding import PartitionSpec as P

HEAD_DIM = 64


norm_eps = 1e-05
tanh_coef = 0.7978845608028654
cube_coef = 0.044715
block_rows = 512


def gelu_tanh(values):
    return (
        0.5 * values * (1.0 + jnp.tanh(tanh_coef * (values + cube_coef * values * values * values)))
    )


def norm_parts(rows):
    center = rows - jnp.mean(rows, axis=-1, keepdims=True)
    spread = jnp.mean(center * center, axis=-1, keepdims=True)
    inverse = lax.rsqrt(spread + norm_eps)
    return (center * inverse, inverse)


def norm_back(grad_out, normed, inverse, gain):
    grad_normed = grad_out * gain
    first = jnp.mean(grad_normed, axis=-1, keepdims=True)
    second = jnp.mean(grad_normed * normed, axis=-1, keepdims=True)
    return inverse * (grad_normed - first - normed * second)


def causal_scores(query_block, keys, positions, offset):
    scores = jnp.einsum(
        "qbhe,kbhe->bhqk", query_block, keys, preferred_element_type=jnp.float32
    ) * HEAD_DIM ** (-0.5)
    height = query_block.shape[0]
    row_pos = lax.dynamic_slice_in_dim(positions, offset, height)[:, None]
    col_pos = positions[None, :]
    return jnp.where(col_pos <= row_pos, scores, -1e30)


def attend_forward(queries, keys, values, positions):
    length = keys.shape[0]
    span = min(block_rows, length)
    outputs = []
    totals = []
    for offset in range(0, length, span):
        scores = causal_scores(queries[offset : offset + span], keys, positions, offset)
        peak = jnp.max(scores, axis=-1, keepdims=True)
        raised = jnp.exp(scores - peak)
        total = jnp.sum(raised, axis=-1, keepdims=True)
        weights = (raised / total).astype(jnp.bfloat16)
        outputs.append(
            jnp.einsum("bhqk,kbhe->qbhe", weights, values, preferred_element_type=jnp.float32)
        )
        totals.append(peak + jnp.log(total))
    return (jnp.concatenate(outputs, 0), jnp.concatenate(totals, 2))


def attend_backward(queries, keys, values, log_totals, grad_out, positions):
    length = keys.shape[0]
    span = min(block_rows, length)
    scale = HEAD_DIM ** (-0.5)
    grad_queries = []
    grad_keys = jnp.zeros(keys.shape, jnp.float32)
    grad_values = jnp.zeros(values.shape, jnp.float32)
    for offset in range(0, length, span):
        query_block = queries[offset : offset + span]
        grad_block = grad_out[offset : offset + span]
        scores = causal_scores(query_block, keys, positions, offset)
        probs = jnp.exp(scores - log_totals[:, :, offset : offset + span])
        grad_probs = jnp.einsum(
            "qbhe,kbhe->bhqk", grad_block, values, preferred_element_type=jnp.float32
        )
        inner = jnp.sum(probs * grad_probs, axis=-1, keepdims=True)
        grad_scores = (probs * (grad_probs - inner)).astype(jnp.bfloat16)
        grad_queries.append(
            jnp.einsum("bhqk,kbhe->qbhe", grad_scores, keys, preferred_element_type=jnp.float32)
            * scale
        )
        grad_keys = (
            grad_keys
            + jnp.einsum(
                "bhqk,qbhe->kbhe", grad_scores, query_block, preferred_element_type=jnp.float32
            )
            * scale
        )
        grad_values = grad_values + jnp.einsum(
            "bhqk,qbhe->kbhe",
            probs.astype(jnp.bfloat16),
            grad_block,
            preferred_element_type=jnp.float32,
        )
    return (jnp.concatenate(grad_queries, 0), grad_keys, grad_values)


SWAP = [(0, 1), (1, 0)]


BLOCK_XOR = (0, 2, 1, 3)


def tensor_gather(block):
    pair = jnp.concatenate([block, lax.ppermute(block, "tx", SWAP)])
    return jnp.concatenate([pair, lax.ppermute(pair, "tc", SWAP)])


def tensor_scatter(parts, send_dtype):
    rows = parts.shape[0] // 4
    got = lax.ppermute(parts[2 * rows :].astype(send_dtype), "tc", SWAP)
    chip = parts[: 2 * rows] + got.astype(jnp.float32)
    got2 = lax.ppermute(chip[rows:].astype(send_dtype), "tx", SWAP)
    return chip[:rows] + got2.astype(jnp.float32)


def block_positions(rows):
    own = lax.axis_index("tx") * 2 + lax.axis_index("tc")
    starts = jnp.bitwise_xor(own, jnp.array(BLOCK_XOR, jnp.int32)) * rows
    return (starts[:, None] + jnp.arange(rows, dtype=jnp.int32)[None, :]).reshape(-1)


def tensor_sum(vector):
    vector = vector + lax.ppermute(vector, "tc", SWAP)
    return vector + lax.ppermute(vector, "tx", SWAP)


def one_micro(resid_in, grad_top, grad_top_full, weights, params):
    qkv_full, out_full, fc_full, proj_full = weights
    qv_bias, out_bias, fc_bias, proj_bias, norm1_gain, norm1_shift, norm2_gain, norm2_shift = params
    heads_local = qkv_full.shape[2] // HEAD_DIM
    normed1, inverse1 = norm_parts(resid_in)
    hidden1 = (normed1 * norm1_gain + norm1_shift).astype(jnp.bfloat16)
    hidden1_full = tensor_gather(hidden1)
    length = hidden1_full.shape[0]
    batch = hidden1_full.shape[1]
    projected = jnp.einsum(
        "lbd,dce->lbce", hidden1_full, qkv_full, preferred_element_type=jnp.float32
    )
    qkv_bias = jnp.stack([qv_bias[0], jnp.zeros_like(qv_bias[0]), qv_bias[1]])
    qkv_values = (projected + qkv_bias).astype(jnp.bfloat16)
    split = qkv_values.reshape(length, batch, 3, heads_local, HEAD_DIM)
    queries = split[:, :, 0]
    keys = split[:, :, 1]
    values = split[:, :, 2]
    positions = block_positions(resid_in.shape[0])
    attended, log_totals = attend_forward(queries, keys, values, positions)
    mixed = attended.astype(jnp.bfloat16).reshape(length, batch, heads_local * HEAD_DIM)
    attn_branch = tensor_scatter(
        jnp.einsum("lbi,oi->lbo", mixed, out_full, preferred_element_type=jnp.float32),
        jnp.float32,
    )
    middle = resid_in + attn_branch + out_bias
    normed2, inverse2 = norm_parts(middle)
    hidden2 = (normed2 * norm2_gain + norm2_shift).astype(jnp.bfloat16)
    hidden2_full = tensor_gather(hidden2)
    pre_act = (
        jnp.einsum("lbd,df->lbf", hidden2_full, fc_full, preferred_element_type=jnp.float32)
        + fc_bias
    )
    activated = gelu_tanh(pre_act).astype(jnp.bfloat16)
    mlp_branch = tensor_scatter(
        jnp.einsum("lbf,of->lbo", activated, proj_full, preferred_element_type=jnp.float32),
        jnp.bfloat16,
    )
    block_out = (middle + mlp_branch + proj_bias).astype(jnp.bfloat16)
    grad_proj = jnp.einsum(
        "lbo,lbf->of", grad_top_full, activated, preferred_element_type=jnp.float32
    )
    grad_act = jnp.einsum(
        "lbo,of->lbf", grad_top_full, proj_full, preferred_element_type=jnp.float32
    )
    _, gelu_pull = jax.vjp(gelu_tanh, pre_act)
    grad_pre = gelu_pull(grad_act)[0].astype(jnp.bfloat16)
    grad_fc_bias = jnp.sum(grad_pre.astype(jnp.float32), axis=(0, 1))
    grad_fc = jnp.einsum(
        "lbd,lbf->df", hidden2_full, grad_pre, preferred_element_type=jnp.float32
    )
    grad_h2 = tensor_scatter(
        jnp.einsum("lbf,df->lbd", grad_pre, fc_full, preferred_element_type=jnp.float32),
        jnp.float32,
    )
    grad_gain2 = jnp.sum(grad_h2 * normed2, axis=(0, 1))
    grad_shift2 = jnp.sum(grad_h2, axis=(0, 1))
    grad_mid = grad_top.astype(jnp.float32) + norm_back(grad_h2, normed2, inverse2, norm2_gain)
    grad_out_bias = jnp.sum(grad_mid, axis=(0, 1))
    grad_proj_bias = jnp.sum(grad_top.astype(jnp.float32), axis=(0, 1))
    grad_mid_full = tensor_gather(grad_mid.astype(jnp.bfloat16))
    grad_out_w = jnp.einsum(
        "lbo,lbi->oi", grad_mid_full, mixed, preferred_element_type=jnp.float32
    )
    grad_mixed = jnp.einsum(
        "lbo,oi->lbi", grad_mid_full, out_full, preferred_element_type=jnp.float32
    )
    grad_mixed = grad_mixed.astype(jnp.bfloat16).reshape(length, batch, heads_local, HEAD_DIM)
    grad_queries, grad_keys, grad_values = attend_backward(
        queries, keys, values, log_totals, grad_mixed, positions
    )
    grad_qkv = jnp.stack([grad_queries, grad_keys, grad_values], axis=2).astype(jnp.bfloat16)
    grad_qkv = grad_qkv.reshape(length, batch, 3, heads_local * HEAD_DIM)
    kind_sums = jnp.sum(grad_qkv.astype(jnp.float32), axis=(0, 1))
    grad_qv_bias = jnp.stack([kind_sums[0], kind_sums[2]])
    grad_qkv_w = jnp.einsum(
        "lbd,lbce->dce", hidden1_full, grad_qkv, preferred_element_type=jnp.float32
    )
    grad_h1 = tensor_scatter(
        jnp.einsum("lbce,dce->lbd", grad_qkv, qkv_full, preferred_element_type=jnp.float32),
        jnp.float32,
    )
    grad_gain1 = jnp.sum(grad_h1 * normed1, axis=(0, 1))
    grad_shift1 = jnp.sum(grad_h1, axis=(0, 1))
    grad_in = (grad_mid + norm_back(grad_h1, normed1, inverse1, norm1_gain)).astype(
        jnp.bfloat16
    )
    depth = qkv_full.shape[0]
    mlp_grads = jnp.concatenate([grad_fc, grad_proj], axis=1)
    attn_grads = jnp.concatenate([grad_qkv_w.reshape(depth, -1), grad_out_w], axis=1)
    head_sums = jnp.concatenate([grad_qv_bias.reshape(-1), grad_fc_bias])
    feature_sums = jnp.concatenate(
        [grad_out_bias, grad_proj_bias, grad_gain1, grad_shift1, grad_gain2, grad_shift2]
    )
    return block_out, grad_in, mlp_grads, attn_grads, head_sums, feature_sums


def per_device(
    block_input,
    qkv_weight,
    qv_bias,
    out_weight,
    out_bias,
    fc_weight,
    fc_bias,
    proj_weight,
    proj_bias,
    norm1_gain,
    norm1_shift,
    norm2_gain,
    norm2_shift,
    out_grad,
):
    micro = block_input.shape[0]
    rows = qkv_weight.shape[0]
    width_qkv = qkv_weight.shape[1] * qkv_weight.shape[2]
    width_fc = fc_weight.shape[1]
    attn_pack = jnp.concatenate([qkv_weight.reshape(rows, width_qkv), out_weight], axis=1)
    mlp_pack = jnp.concatenate([fc_weight, proj_weight], axis=1)
    attn_full = lax.all_gather(attn_pack, "dp", axis=0, tiled=True)
    mlp_full = lax.all_gather(mlp_pack, "dp", axis=0, tiled=True)
    depth = attn_full.shape[0]
    weights = (
        attn_full[:, :width_qkv].reshape(depth, 3, qkv_weight.shape[2]),
        attn_full[:, width_qkv:],
        mlp_full[:, :width_fc],
        mlp_full[:, width_fc:],
    )
    params = (qv_bias, out_bias, fc_bias, proj_bias, norm1_gain, norm1_shift, norm2_gain, norm2_shift)
    grad_top_all = jnp.swapaxes(tensor_gather(jnp.swapaxes(out_grad, 0, 1)), 0, 1)
    outputs, in_grads = [], []
    mlp_acc = attn_acc = head_acc = feature_acc = None
    for index in range(micro):
        block_out, grad_in, mlp_grads, attn_grads, head_sums, feature_sums = one_micro(
            block_input[index].astype(jnp.float32),
            out_grad[index],
            grad_top_all[index],
            weights,
            params,
        )
        outputs.append(block_out)
        in_grads.append(grad_in)
        if index == 0:
            mlp_acc, attn_acc, head_acc, feature_acc = mlp_grads, attn_grads, head_sums, feature_sums
        else:
            mlp_acc = mlp_acc + mlp_grads
            attn_acc = attn_acc + attn_grads
            head_acc = head_acc + head_sums
            feature_acc = feature_acc + feature_sums
    mlp_shard = lax.psum_scatter(mlp_acc, "dp", scatter_dimension=0, tiled=True)
    small = jnp.concatenate([tensor_sum(feature_acc), head_acc])
    width_attn = attn_acc.shape[1]
    small_rows = -(-small.shape[0] // width_attn)
    small = jnp.pad(small, (0, small_rows * width_attn - small.shape[0])).reshape(
        small_rows, width_attn
    )
    blocks = depth // rows
    attn_rows = jnp.concatenate(
        [
            attn_acc.reshape(blocks, rows, width_attn),
            jnp.broadcast_to(small, (blocks, small_rows, width_attn)),
        ],
        axis=1,
    ).reshape(blocks * (rows + small_rows), width_attn)
    attn_shard = lax.psum_scatter(attn_rows, "dp", scatter_dimension=0, tiled=True)
    small_total = attn_shard[rows:].reshape(-1)
    features = small_total[: feature_acc.shape[0]].reshape(6, -1)
    head_total = small_total[feature_acc.shape[0] : feature_acc.shape[0] + head_acc.shape[0]]
    qv_size = qv_bias.size
    return (
        jnp.stack(outputs),
        jnp.stack(in_grads),
        attn_shard[:rows, :width_qkv].reshape(qkv_weight.shape),
        head_total[:qv_size].reshape(qv_bias.shape),
        attn_shard[:rows, width_qkv:],
        features[0],
        mlp_shard[:, :width_fc],
        head_total[qv_size:],
        mlp_shard[:, width_fc:],
        features[1],
        features[2],
        features[3],
        features[4],
        features[5],
    )


def solution(mesh):
    assert mesh.shape["tensor"] == 4
    devices = mesh.devices.reshape(mesh.shape["dp"], 2, 2)
    mesh = jax.sharding.Mesh(devices, ("dp", "tx", "tc"))
    in_specs = (
        P(None, ("tx", "tc"), "dp", None),
        P("dp", None, ("tx", "tc")),
        P(None, ("tx", "tc")),
        P("dp", ("tx", "tc")),
        P(),
        P("dp", ("tx", "tc")),
        P(("tx", "tc")),
        P("dp", ("tx", "tc")),
        P(),
        P(),
        P(),
        P(),
        P(),
        P(None, ("tx", "tc"), "dp", None),
    )
    out_specs = (
        P(None, ("tx", "tc"), "dp", None),
        P(None, ("tx", "tc"), "dp", None),
        P("dp", None, ("tx", "tc")),
        P(None, ("tx", "tc")),
        P("dp", ("tx", "tc")),
        P(),
        P("dp", ("tx", "tc")),
        P(("tx", "tc")),
        P("dp", ("tx", "tc")),
        P(),
        P(),
        P(),
        P(),
        P(),
    )
    return jax.shard_map(
        per_device, mesh=mesh, in_specs=in_specs, out_specs=out_specs, check_vma=False
    )
```

```python
import jax
import jax.numpy as jnp
from jax import lax
from jax.sharding import PartitionSpec as P

HEAD_DIM = 64


norm_eps = 1e-05
tanh_coef = 0.7978845608028654
cube_coef = 0.044715
block_rows = 512


def gelu_tanh(values):
    return (
        0.5 * values * (1.0 + jnp.tanh(tanh_coef * (values + cube_coef * values * values * values)))
    )


def norm_parts(rows):
    center = rows - jnp.mean(rows, axis=-1, keepdims=True)
    spread = jnp.mean(center * center, axis=-1, keepdims=True)
    inverse = lax.rsqrt(spread + norm_eps)
    return (center * inverse, inverse)


def norm_back(grad_out, normed, inverse, gain):
    grad_normed = grad_out * gain
    first = jnp.mean(grad_normed, axis=-1, keepdims=True)
    second = jnp.mean(grad_normed * normed, axis=-1, keepdims=True)
    return inverse * (grad_normed - first - normed * second)


def causal_scores(query_block, keys, positions, offset):
    scores = jnp.einsum(
        "qbhe,kbhe->bhqk", query_block, keys, preferred_element_type=jnp.float32
    ) * HEAD_DIM ** (-0.5)
    height = query_block.shape[0]
    row_pos = lax.dynamic_slice_in_dim(positions, offset, height)[:, None]
    col_pos = positions[None, :]
    return jnp.where(col_pos <= row_pos, scores, -1e30)


def attend_forward(queries, keys, values, positions):
    length = keys.shape[0]
    span = min(block_rows, length)
    outputs = []
    totals = []
    for offset in range(0, length, span):
        scores = causal_scores(queries[offset : offset + span], keys, positions, offset)
        peak = jnp.max(scores, axis=-1, keepdims=True)
        raised = jnp.exp(scores - peak)
        total = jnp.sum(raised, axis=-1, keepdims=True)
        weights = (raised / total).astype(jnp.bfloat16)
        outputs.append(
            jnp.einsum("bhqk,kbhe->qbhe", weights, values, preferred_element_type=jnp.float32)
        )
        totals.append(peak + jnp.log(total))
    return (jnp.concatenate(outputs, 0), jnp.concatenate(totals, 2))


def attend_backward(queries, keys, values, log_totals, grad_out, positions):
    length = keys.shape[0]
    span = min(block_rows, length)
    scale = HEAD_DIM ** (-0.5)
    grad_queries = []
    grad_keys = jnp.zeros(keys.shape, jnp.float32)
    grad_values = jnp.zeros(values.shape, jnp.float32)
    for offset in range(0, length, span):
        query_block = queries[offset : offset + span]
        grad_block = grad_out[offset : offset + span]
        scores = causal_scores(query_block, keys, positions, offset)
        probs = jnp.exp(scores - log_totals[:, :, offset : offset + span])
        grad_probs = jnp.einsum(
            "qbhe,kbhe->bhqk", grad_block, values, preferred_element_type=jnp.float32
        )
        inner = jnp.sum(probs * grad_probs, axis=-1, keepdims=True)
        grad_scores = (probs * (grad_probs - inner)).astype(jnp.bfloat16)
        grad_queries.append(
            jnp.einsum("bhqk,kbhe->qbhe", grad_scores, keys, preferred_element_type=jnp.float32)
            * scale
        )
        grad_keys = (
            grad_keys
            + jnp.einsum(
                "bhqk,qbhe->kbhe", grad_scores, query_block, preferred_element_type=jnp.float32
            )
            * scale
        )
        grad_values = grad_values + jnp.einsum(
            "bhqk,qbhe->kbhe",
            probs.astype(jnp.bfloat16),
            grad_block,
            preferred_element_type=jnp.float32,
        )
    return (jnp.concatenate(grad_queries, 0), grad_keys, grad_values)


SWAP = [(0, 1), (1, 0)]


BLOCK_XOR = (0, 2, 1, 3)


def tensor_gather(block):
    pair = jnp.concatenate([block, lax.ppermute(block, "tx", SWAP)])
    return jnp.concatenate([pair, lax.ppermute(pair, "tc", SWAP)])


def tensor_scatter(parts, send_dtype):
    rows = parts.shape[0] // 4
    got = lax.ppermute(parts[2 * rows :].astype(send_dtype), "tc", SWAP)
    chip = parts[: 2 * rows] + got.astype(jnp.float32)
    got2 = lax.ppermute(chip[rows:].astype(send_dtype), "tx", SWAP)
    return chip[:rows] + got2.astype(jnp.float32)


def block_positions(rows):
    own = lax.axis_index("tx") * 2 + lax.axis_index("tc")
    starts = jnp.bitwise_xor(own, jnp.array(BLOCK_XOR, jnp.int32)) * rows
    return (starts[:, None] + jnp.arange(rows, dtype=jnp.int32)[None, :]).reshape(-1)


def tensor_sum(vector):
    vector = vector + lax.ppermute(vector, "tc", SWAP)
    return vector + lax.ppermute(vector, "tx", SWAP)


def one_micro(resid_in, grad_top, grad_top_full, weights, params):
    qkv_full, out_full, fc_full, proj_full = weights
    qv_bias, out_bias, fc_bias, proj_bias, norm1_gain, norm1_shift, norm2_gain, norm2_shift = params
    heads_local = qkv_full.shape[2] // HEAD_DIM
    normed1, inverse1 = norm_parts(resid_in)
    hidden1 = (normed1 * norm1_gain + norm1_shift).astype(jnp.bfloat16)
    hidden1_full = tensor_gather(hidden1)
    length = hidden1_full.shape[0]
    batch = hidden1_full.shape[1]
    projected = jnp.einsum(
        "lbd,dce->lbce", hidden1_full, qkv_full, preferred_element_type=jnp.float32
    )
    qkv_bias = jnp.stack([qv_bias[0], jnp.zeros_like(qv_bias[0]), qv_bias[1]])
    qkv_values = (projected + qkv_bias).astype(jnp.bfloat16)
    split = qkv_values.reshape(length, batch, 3, heads_local, HEAD_DIM)
    queries = split[:, :, 0]
    keys = split[:, :, 1]
    values = split[:, :, 2]
    positions = block_positions(resid_in.shape[0])
    attended, log_totals = attend_forward(queries, keys, values, positions)
    mixed = attended.astype(jnp.bfloat16).reshape(length, batch, heads_local * HEAD_DIM)
    attn_branch = tensor_scatter(
        jnp.einsum("lbi,oi->lbo", mixed, out_full, preferred_element_type=jnp.float32),
        jnp.bfloat16,
    )
    middle = resid_in + attn_branch + out_bias
    normed2, inverse2 = norm_parts(middle)
    hidden2 = (normed2 * norm2_gain + norm2_shift).astype(jnp.bfloat16)
    hidden2_full = tensor_gather(hidden2)
    pre_act = (
        jnp.einsum("lbd,df->lbf", hidden2_full, fc_full, preferred_element_type=jnp.float32)
        + fc_bias
    )
    activated = gelu_tanh(pre_act).astype(jnp.bfloat16)
    mlp_branch = tensor_scatter(
        jnp.einsum("lbf,of->lbo", activated, proj_full, preferred_element_type=jnp.float32),
        jnp.bfloat16,
    )
    block_out = (middle + mlp_branch + proj_bias).astype(jnp.bfloat16)
    grad_proj = jnp.einsum(
        "lbo,lbf->of", grad_top_full, activated, preferred_element_type=jnp.float32
    )
    grad_act = jnp.einsum(
        "lbo,of->lbf", grad_top_full, proj_full, preferred_element_type=jnp.float32
    )
    _, gelu_pull = jax.vjp(gelu_tanh, pre_act)
    grad_pre = gelu_pull(grad_act)[0].astype(jnp.bfloat16)
    grad_fc_bias = jnp.sum(grad_pre.astype(jnp.float32), axis=(0, 1))
    grad_fc = jnp.einsum(
        "lbd,lbf->df", hidden2_full, grad_pre, preferred_element_type=jnp.float32
    )
    grad_h2 = tensor_scatter(
        jnp.einsum("lbf,df->lbd", grad_pre, fc_full, preferred_element_type=jnp.float32),
        jnp.bfloat16,
    )
    grad_gain2 = jnp.sum(grad_h2 * normed2, axis=(0, 1))
    grad_shift2 = jnp.sum(grad_h2, axis=(0, 1))
    grad_mid = grad_top.astype(jnp.float32) + norm_back(grad_h2, normed2, inverse2, norm2_gain)
    grad_out_bias = jnp.sum(grad_mid, axis=(0, 1))
    grad_proj_bias = jnp.sum(grad_top.astype(jnp.float32), axis=(0, 1))
    grad_mid_full = tensor_gather(grad_mid.astype(jnp.bfloat16))
    grad_out_w = jnp.einsum(
        "lbo,lbi->oi", grad_mid_full, mixed, preferred_element_type=jnp.float32
    )
    grad_mixed = jnp.einsum(
        "lbo,oi->lbi", grad_mid_full, out_full, preferred_element_type=jnp.float32
    )
    grad_mixed = grad_mixed.astype(jnp.bfloat16).reshape(length, batch, heads_local, HEAD_DIM)
    grad_queries, grad_keys, grad_values = attend_backward(
        queries, keys, values, log_totals, grad_mixed, positions
    )
    grad_qkv = jnp.stack([grad_queries, grad_keys, grad_values], axis=2).astype(jnp.bfloat16)
    grad_qkv = grad_qkv.reshape(length, batch, 3, heads_local * HEAD_DIM)
    kind_sums = jnp.sum(grad_qkv.astype(jnp.float32), axis=(0, 1))
    grad_qv_bias = jnp.stack([kind_sums[0], kind_sums[2]])
    grad_qkv_w = jnp.einsum(
        "lbd,lbce->dce", hidden1_full, grad_qkv, preferred_element_type=jnp.float32
    )
    grad_h1 = tensor_scatter(
        jnp.einsum("lbce,dce->lbd", grad_qkv, qkv_full, preferred_element_type=jnp.float32),
        jnp.bfloat16,
    )
    grad_gain1 = jnp.sum(grad_h1 * normed1, axis=(0, 1))
    grad_shift1 = jnp.sum(grad_h1, axis=(0, 1))
    grad_in = (grad_mid + norm_back(grad_h1, normed1, inverse1, norm1_gain)).astype(
        jnp.bfloat16
    )
    depth = qkv_full.shape[0]
    mlp_grads = jnp.concatenate([grad_fc, grad_proj], axis=1)
    attn_grads = jnp.concatenate([grad_qkv_w.reshape(depth, -1), grad_out_w], axis=1)
    head_sums = jnp.concatenate([grad_qv_bias.reshape(-1), grad_fc_bias])
    feature_sums = jnp.concatenate(
        [grad_out_bias, grad_proj_bias, grad_gain1, grad_shift1, grad_gain2, grad_shift2]
    )
    return block_out, grad_in, mlp_grads, attn_grads, head_sums, feature_sums


def per_device(
    block_input,
    qkv_weight,
    qv_bias,
    out_weight,
    out_bias,
    fc_weight,
    fc_bias,
    proj_weight,
    proj_bias,
    norm1_gain,
    norm1_shift,
    norm2_gain,
    norm2_shift,
    out_grad,
):
    micro = block_input.shape[0]
    rows = qkv_weight.shape[0]
    width_qkv = qkv_weight.shape[1] * qkv_weight.shape[2]
    width_fc = fc_weight.shape[1]
    attn_pack = jnp.concatenate([qkv_weight.reshape(rows, width_qkv), out_weight], axis=1)
    mlp_pack = jnp.concatenate([fc_weight, proj_weight], axis=1)
    attn_full = lax.all_gather(attn_pack, "dp", axis=0, tiled=True)
    mlp_full = lax.all_gather(mlp_pack, "dp", axis=0, tiled=True)
    depth = attn_full.shape[0]
    weights = (
        attn_full[:, :width_qkv].reshape(depth, 3, qkv_weight.shape[2]),
        attn_full[:, width_qkv:],
        mlp_full[:, :width_fc],
        mlp_full[:, width_fc:],
    )
    params = (qv_bias, out_bias, fc_bias, proj_bias, norm1_gain, norm1_shift, norm2_gain, norm2_shift)
    grad_top_all = jnp.swapaxes(tensor_gather(jnp.swapaxes(out_grad, 0, 1)), 0, 1)
    outputs, in_grads = [], []
    mlp_acc = attn_acc = head_acc = feature_acc = None
    for index in range(micro):
        block_out, grad_in, mlp_grads, attn_grads, head_sums, feature_sums = one_micro(
            block_input[index].astype(jnp.float32),
            out_grad[index],
            grad_top_all[index],
            weights,
            params,
        )
        outputs.append(block_out)
        in_grads.append(grad_in)
        if index == 0:
            mlp_acc, attn_acc, head_acc, feature_acc = mlp_grads, attn_grads, head_sums, feature_sums
        else:
            mlp_acc = mlp_acc + mlp_grads
            attn_acc = attn_acc + attn_grads
            head_acc = head_acc + head_sums
            feature_acc = feature_acc + feature_sums
    mlp_shard = lax.psum_scatter(mlp_acc, "dp", scatter_dimension=0, tiled=True)
    small = jnp.concatenate([tensor_sum(feature_acc), head_acc])
    width_attn = attn_acc.shape[1]
    small_rows = -(-small.shape[0] // width_attn)
    small = jnp.pad(small, (0, small_rows * width_attn - small.shape[0])).reshape(
        small_rows, width_attn
    )
    blocks = depth // rows
    attn_rows = jnp.concatenate(
        [
            attn_acc.reshape(blocks, rows, width_attn),
            jnp.broadcast_to(small, (blocks, small_rows, width_attn)),
        ],
        axis=1,
    ).reshape(blocks * (rows + small_rows), width_attn)
    attn_shard = lax.psum_scatter(attn_rows, "dp", scatter_dimension=0, tiled=True)
    small_total = attn_shard[rows:].reshape(-1)
    features = small_total[: feature_acc.shape[0]].reshape(6, -1)
    head_total = small_total[feature_acc.shape[0] : feature_acc.shape[0] + head_acc.shape[0]]
    qv_size = qv_bias.size
    return (
        jnp.stack(outputs),
        jnp.stack(in_grads),
        attn_shard[:rows, :width_qkv].reshape(qkv_weight.shape),
        head_total[:qv_size].reshape(qv_bias.shape),
        attn_shard[:rows, width_qkv:],
        features[0],
        mlp_shard[:, :width_fc],
        head_total[qv_size:],
        mlp_shard[:, width_fc:],
        features[1],
        features[2],
        features[3],
        features[4],
        features[5],
    )


def solution(mesh):
    assert mesh.shape["tensor"] == 4
    devices = mesh.devices.reshape(mesh.shape["dp"], 2, 2)
    mesh = jax.sharding.Mesh(devices, ("dp", "tx", "tc"))
    in_specs = (
        P(None, ("tx", "tc"), "dp", None),
        P("dp", None, ("tx", "tc")),
        P(None, ("tx", "tc")),
        P("dp", ("tx", "tc")),
        P(),
        P("dp", ("tx", "tc")),
        P(("tx", "tc")),
        P("dp", ("tx", "tc")),
        P(),
        P(),
        P(),
        P(),
        P(),
        P(None, ("tx", "tc"), "dp", None),
    )
    out_specs = (
        P(None, ("tx", "tc"), "dp", None),
        P(None, ("tx", "tc"), "dp", None),
        P("dp", None, ("tx", "tc")),
        P(None, ("tx", "tc")),
        P("dp", ("tx", "tc")),
        P(),
        P("dp", ("tx", "tc")),
        P(("tx", "tc")),
        P("dp", ("tx", "tc")),
        P(),
        P(),
        P(),
        P(),
        P(),
    )
    return jax.shard_map(
        per_device, mesh=mesh, in_specs=in_specs, out_specs=out_specs, check_vma=False
    )
```

```python
import jax
import jax.numpy as jnp
from jax import lax
from jax.sharding import PartitionSpec as P


HEAD_DIM = 64


norm_eps = 1e-05
tanh_coef = 0.7978845608028654
cube_coef = 0.044715
block_rows = 512


def gelu_tanh(values):
    return (
        0.5 * values * (1.0 + jnp.tanh(tanh_coef * (values + cube_coef * values * values * values)))
    )


def norm_parts(rows):
    center = rows - jnp.mean(rows, axis=-1, keepdims=True)
    spread = jnp.mean(center * center, axis=-1, keepdims=True)
    inverse = lax.rsqrt(spread + norm_eps)
    return (center * inverse, inverse)


def norm_back(grad_out, normed, inverse, gain):
    grad_normed = grad_out * gain
    first = jnp.mean(grad_normed, axis=-1, keepdims=True)
    second = jnp.mean(grad_normed * normed, axis=-1, keepdims=True)
    return inverse * (grad_normed - first - normed * second)


def causal_scores(query_block, keys, positions, offset):
    scores = jnp.einsum(
        "qbhe,kbhe->bhqk", query_block, keys, preferred_element_type=jnp.float32
    ) * HEAD_DIM ** (-0.5)
    height = query_block.shape[0]
    row_pos = lax.dynamic_slice_in_dim(positions, offset, height)[:, None]
    col_pos = positions[None, :]
    return jnp.where(col_pos <= row_pos, scores, -1e30)


def attend_forward(queries, keys, values, positions):
    length = keys.shape[0]
    span = min(block_rows, length)
    outputs = []
    totals = []
    for offset in range(0, length, span):
        scores = causal_scores(queries[offset : offset + span], keys, positions, offset)
        peak = jnp.max(scores, axis=-1, keepdims=True)
        raised = jnp.exp(scores - peak)
        total = jnp.sum(raised, axis=-1, keepdims=True)
        weights = (raised / total).astype(jnp.bfloat16)
        outputs.append(
            jnp.einsum("bhqk,kbhe->qbhe", weights, values, preferred_element_type=jnp.float32)
        )
        totals.append(peak + jnp.log(total))
    return (jnp.concatenate(outputs, 0), jnp.concatenate(totals, 2))


def attend_backward(queries, keys, values, log_totals, grad_out, positions):
    length = keys.shape[0]
    span = min(block_rows, length)
    scale = HEAD_DIM ** (-0.5)
    grad_queries = []
    grad_keys = jnp.zeros(keys.shape, jnp.float32)
    grad_values = jnp.zeros(values.shape, jnp.float32)
    for offset in range(0, length, span):
        query_block = queries[offset : offset + span]
        grad_block = grad_out[offset : offset + span]
        scores = causal_scores(query_block, keys, positions, offset)
        probs = jnp.exp(scores - log_totals[:, :, offset : offset + span])
        grad_probs = jnp.einsum(
            "qbhe,kbhe->bhqk", grad_block, values, preferred_element_type=jnp.float32
        )
        inner = jnp.sum(probs * grad_probs, axis=-1, keepdims=True)
        grad_scores = (probs * (grad_probs - inner)).astype(jnp.bfloat16)
        grad_queries.append(
            jnp.einsum("bhqk,kbhe->qbhe", grad_scores, keys, preferred_element_type=jnp.float32)
            * scale
        )
        grad_keys = (
            grad_keys
            + jnp.einsum(
                "bhqk,qbhe->kbhe", grad_scores, query_block, preferred_element_type=jnp.float32
            )
            * scale
        )
        grad_values = grad_values + jnp.einsum(
            "bhqk,qbhe->kbhe",
            probs.astype(jnp.bfloat16),
            grad_block,
            preferred_element_type=jnp.float32,
        )
    return (jnp.concatenate(grad_queries, 0), grad_keys, grad_values)


SWAP = [(0, 1), (1, 0)]


BLOCK_XOR = (0, 2, 1, 3)


def tensor_gather(block):
    pair = jnp.concatenate([block, lax.ppermute(block, "tx", SWAP)])
    return jnp.concatenate([pair, lax.ppermute(pair, "tc", SWAP)])


def tensor_scatter(parts, send_dtype):
    rows = parts.shape[0] // 4
    got = lax.ppermute(parts[2 * rows :].astype(send_dtype), "tc", SWAP)
    chip = parts[: 2 * rows] + got.astype(jnp.float32)
    got2 = lax.ppermute(chip[rows:].astype(send_dtype), "tx", SWAP)
    return chip[:rows] + got2.astype(jnp.float32)


def block_positions(rows):
    own = lax.axis_index("tx") * 2 + lax.axis_index("tc")
    starts = jnp.bitwise_xor(own, jnp.array(BLOCK_XOR, jnp.int32)) * rows
    return (starts[:, None] + jnp.arange(rows, dtype=jnp.int32)[None, :]).reshape(-1)


def tensor_sum(vector):
    vector = vector + lax.ppermute(vector, "tc", SWAP)
    return vector + lax.ppermute(vector, "tx", SWAP)


def one_micro(resid_in, grad_top, grad_top_full, weights, params):
    qkv_full, out_full, fc_full, proj_full = weights
    qv_bias, out_bias, fc_bias, proj_bias, norm1_gain, norm1_shift, norm2_gain, norm2_shift = params
    heads_local = qkv_full.shape[2] // HEAD_DIM
    normed1, inverse1 = norm_parts(resid_in)
    hidden1 = (normed1 * norm1_gain + norm1_shift).astype(jnp.bfloat16)
    hidden1_full = tensor_gather(hidden1)
    length = hidden1_full.shape[0]
    batch = hidden1_full.shape[1]
    projected = jnp.einsum(
        "lbd,dce->lbce", hidden1_full, qkv_full, preferred_element_type=jnp.float32
    )
    qkv_bias = jnp.stack([qv_bias[0], jnp.zeros_like(qv_bias[0]), qv_bias[1]])
    qkv_values = (projected + qkv_bias).astype(jnp.bfloat16)
    split = qkv_values.reshape(length, batch, 3, heads_local, HEAD_DIM)
    queries = split[:, :, 0]
    keys = split[:, :, 1]
    values = split[:, :, 2]
    positions = block_positions(resid_in.shape[0])
    attended, log_totals = attend_forward(queries, keys, values, positions)
    mixed = attended.astype(jnp.bfloat16).reshape(length, batch, heads_local * HEAD_DIM)
    attn_branch = tensor_scatter(
        jnp.einsum("lbi,oi->lbo", mixed, out_full, preferred_element_type=jnp.float32),
        jnp.bfloat16,
    )
    middle = resid_in + attn_branch + out_bias
    normed2, inverse2 = norm_parts(middle)
    hidden2 = (normed2 * norm2_gain + norm2_shift).astype(jnp.bfloat16)
    hidden2_full = tensor_gather(hidden2)
    pre_act = (
        jnp.einsum("lbd,df->lbf", hidden2_full, fc_full, preferred_element_type=jnp.float32)
        + fc_bias
    )
    activated = gelu_tanh(pre_act).astype(jnp.bfloat16)
    mlp_branch = tensor_scatter(
        jnp.einsum("lbf,of->lbo", activated, proj_full, preferred_element_type=jnp.float32),
        jnp.bfloat16,
    )
    block_out = (middle + mlp_branch + proj_bias).astype(jnp.bfloat16)
    grad_proj = jnp.einsum(
        "lbo,lbf->of", grad_top_full, activated, preferred_element_type=jnp.float32
    )
    grad_act = jnp.einsum(
        "lbo,of->lbf", grad_top_full, proj_full, preferred_element_type=jnp.float32
    )
    _, gelu_pull = jax.vjp(gelu_tanh, pre_act)
    grad_pre = gelu_pull(grad_act)[0].astype(jnp.bfloat16)
    grad_fc_bias = jnp.sum(grad_pre.astype(jnp.float32), axis=(0, 1))
    grad_fc = jnp.einsum(
        "lbd,lbf->df", hidden2_full, grad_pre, preferred_element_type=jnp.float32
    )
    grad_h2 = tensor_scatter(
        jnp.einsum("lbf,df->lbd", grad_pre, fc_full, preferred_element_type=jnp.float32),
        jnp.bfloat16,
    )
    grad_gain2 = jnp.sum(grad_h2 * normed2, axis=(0, 1))
    grad_shift2 = jnp.sum(grad_h2, axis=(0, 1))
    grad_mid = grad_top.astype(jnp.float32) + norm_back(grad_h2, normed2, inverse2, norm2_gain)
    grad_out_bias = jnp.sum(grad_mid, axis=(0, 1))
    grad_proj_bias = jnp.sum(grad_top.astype(jnp.float32), axis=(0, 1))
    grad_mid_full = tensor_gather(grad_mid.astype(jnp.bfloat16))
    grad_out_w = jnp.einsum(
        "lbo,lbi->oi", grad_mid_full, mixed, preferred_element_type=jnp.float32
    )
    grad_mixed = jnp.einsum(
        "lbo,oi->lbi", grad_mid_full, out_full, preferred_element_type=jnp.float32
    )
    grad_mixed = grad_mixed.astype(jnp.bfloat16).reshape(length, batch, heads_local, HEAD_DIM)
    grad_queries, grad_keys, grad_values = attend_backward(
        queries, keys, values, log_totals, grad_mixed, positions
    )
    grad_qkv = jnp.stack([grad_queries, grad_keys, grad_values], axis=2).astype(jnp.bfloat16)
    grad_qkv = grad_qkv.reshape(length, batch, 3, heads_local * HEAD_DIM)
    kind_sums = jnp.sum(grad_qkv.astype(jnp.float32), axis=(0, 1))
    grad_qv_bias = jnp.stack([kind_sums[0], kind_sums[2]])
    grad_qkv_w = jnp.einsum(
        "lbd,lbce->dce", hidden1_full, grad_qkv, preferred_element_type=jnp.float32
    )
    grad_h1 = tensor_scatter(
        jnp.einsum("lbce,dce->lbd", grad_qkv, qkv_full, preferred_element_type=jnp.float32),
        jnp.bfloat16,
    )
    grad_gain1 = jnp.sum(grad_h1 * normed1, axis=(0, 1))
    grad_shift1 = jnp.sum(grad_h1, axis=(0, 1))
    grad_in = (grad_mid + norm_back(grad_h1, normed1, inverse1, norm1_gain)).astype(
        jnp.bfloat16
    )
    depth = qkv_full.shape[0]
    mlp_grads = jnp.concatenate([grad_fc, grad_proj], axis=1)
    attn_grads = jnp.concatenate([grad_qkv_w.reshape(depth, -1), grad_out_w], axis=1)
    head_sums = jnp.concatenate([grad_qv_bias.reshape(-1), grad_fc_bias])
    feature_sums = jnp.concatenate(
        [grad_out_bias, grad_proj_bias, grad_gain1, grad_shift1, grad_gain2, grad_shift2]
    )
    return block_out, grad_in, mlp_grads, attn_grads, head_sums, feature_sums


def per_device(
    block_input,
    qkv_weight,
    qv_bias,
    out_weight,
    out_bias,
    fc_weight,
    fc_bias,
    proj_weight,
    proj_bias,
    norm1_gain,
    norm1_shift,
    norm2_gain,
    norm2_shift,
    out_grad,
):
    micro = block_input.shape[0]
    rows = qkv_weight.shape[0]
    width_qkv = qkv_weight.shape[1] * qkv_weight.shape[2]
    width_fc = fc_weight.shape[1]
    attn_pack = jnp.concatenate([qkv_weight.reshape(rows, width_qkv), out_weight], axis=1)
    mlp_pack = jnp.concatenate([fc_weight, proj_weight], axis=1)
    attn_full = lax.all_gather(attn_pack, "dp", axis=0, tiled=True)
    mlp_full = lax.all_gather(mlp_pack, "dp", axis=0, tiled=True)
    depth = attn_full.shape[0]
    weights = (
        attn_full[:, :width_qkv].reshape(depth, 3, qkv_weight.shape[2]),
        attn_full[:, width_qkv:],
        mlp_full[:, :width_fc],
        mlp_full[:, width_fc:],
    )
    params = (qv_bias, out_bias, fc_bias, proj_bias, norm1_gain, norm1_shift, norm2_gain, norm2_shift)
    grad_top_all = jnp.swapaxes(tensor_gather(jnp.swapaxes(out_grad, 0, 1)), 0, 1)
    outputs, in_grads = [], []
    mlp_acc = attn_acc = head_acc = feature_acc = None
    for index in range(micro):
        block_out, grad_in, mlp_grads, attn_grads, head_sums, feature_sums = one_micro(
            block_input[index].astype(jnp.float32),
            out_grad[index],
            grad_top_all[index],
            weights,
            params,
        )
        outputs.append(block_out)
        in_grads.append(grad_in)
        if index == 0:
            mlp_acc, attn_acc, head_acc, feature_acc = mlp_grads, attn_grads, head_sums, feature_sums
        else:
            mlp_acc = mlp_acc + mlp_grads
            attn_acc = attn_acc + attn_grads
            head_acc = head_acc + head_sums
            feature_acc = feature_acc + feature_sums
    mlp_shard = lax.psum_scatter(
        mlp_acc.astype(jnp.bfloat16), "dp", scatter_dimension=0, tiled=True
    ).astype(jnp.float32)
    attn_shard = lax.psum_scatter(
        attn_acc.astype(jnp.bfloat16), "dp", scatter_dimension=0, tiled=True
    ).astype(jnp.float32)
    small = jnp.concatenate([tensor_sum(feature_acc), head_acc])
    groups = lax.psum(1, "dp")
    step = 1
    while step < groups:
        small = small + lax.ppermute(small, "dp", [(i, i ^ step) for i in range(groups)])
        step *= 2
    features = small[: feature_acc.shape[0]].reshape(6, -1)
    head_total = small[feature_acc.shape[0] :]
    qv_size = qv_bias.size
    return (
        jnp.stack(outputs),
        jnp.stack(in_grads),
        attn_shard[:, :width_qkv].reshape(qkv_weight.shape),
        head_total[:qv_size].reshape(qv_bias.shape),
        attn_shard[:, width_qkv:],
        features[0],
        mlp_shard[:, :width_fc],
        head_total[qv_size:],
        mlp_shard[:, width_fc:],
        features[1],
        features[2],
        features[3],
        features[4],
        features[5],
    )


def solution(mesh):
    assert mesh.shape["tensor"] == 4
    devices = mesh.devices.reshape(mesh.shape["dp"], 2, 2)
    mesh = jax.sharding.Mesh(devices, ("dp", "tx", "tc"))
    in_specs = (
        P(None, ("tx", "tc"), "dp", None),
        P("dp", None, ("tx", "tc")),
        P(None, ("tx", "tc")),
        P("dp", ("tx", "tc")),
        P(),
        P("dp", ("tx", "tc")),
        P(("tx", "tc")),
        P("dp", ("tx", "tc")),
        P(),
        P(),
        P(),
        P(),
        P(),
        P(None, ("tx", "tc"), "dp", None),
    )
    out_specs = (
        P(None, ("tx", "tc"), "dp", None),
        P(None, ("tx", "tc"), "dp", None),
        P("dp", None, ("tx", "tc")),
        P(None, ("tx", "tc")),
        P("dp", ("tx", "tc")),
        P(),
        P("dp", ("tx", "tc")),
        P(("tx", "tc")),
        P("dp", ("tx", "tc")),
        P(),
        P(),
        P(),
        P(),
        P(),
    )

    return jax.shard_map(
        per_device, mesh=mesh, in_specs=in_specs, out_specs=out_specs, check_vma=False
    )
```
